128 devices in a mesh: tile: 32 (over z, x, core), slab: 4 (over y).
Axes of the slice: x: 4, y: 4, z: 4, core: 2. Of those that a mesh axis runs over, the one named last changes fastest.
Arguments:
- object_field: float32 [2, 2, 16384, 2048], P(None, None, 'tile', 'slab')
- probe: float32 [2, 256, 256], replicated, may hold values from -5 to 5
- kernel_phase: float32 [256, 256], replicated, may hold values from -3.140625 to 3.140625
- measured: float32 [512, 256, 256], P(('tile', 'slab')), may hold values from 0.2 to 2
- positions: int32 [512, 2], P(('tile', 'slab')), may hold values from 0 to 16128, as said below
- batch: int32 [512], P(('tile', 'slab')), may hold values from 0 to 1
Outputs:
- object_new: float32 [2, 2, 16384, 2048], P(None, None, 'tile', 'slab')
- probe_new: float32 [2, 256, 256], replicated
The draws below stay inside these ranges and needn't reach their ends.
Inputs may be any that keep to these rules, and one draw needn't show every extreme that they name: `positions`: frame f's top-left pixel lies in the tile of rows t * 512 .. (t + 1) * 512 - 1 and columns s * 512 .. (s + 1) * 512 - 1, where t = (f // 4) // 4 and s = (f // 4) % 4; every frame lies inside the object.
All inputs are finite; a program needn't handle non-finite values.
Results may differ from the reference program's by a relative error of at most 0.0003.
Values sent between devices are 32-bit elements; how exact they have to be, the bound alone decides.
A program may use at most 192 MiB of HBM per device.

```python
import math
import jax
import jax.numpy as jnp
from jax import lax

K = 256
LAYERS = 2
BATCHES = 2
TR = 512
TC = 512
F_DEV = 4
ROW_TILES = 32
COL_TILES = 4
NR = 16384
NC = 2048
FRAMES = 512


def draw_object_field(key, part):
    key_amp, key_phase = jax.random.split(jax.random.fold_in(key, 101))
    shape = (LAYERS, NR, NC)
    amplitude = jax.random.uniform(key_amp, shape, jnp.float32, 0.6, 1.2)
    phase = jax.random.uniform(key_phase, shape, jnp.float32, -math.pi, math.pi)
    return jnp.stack([amplitude * jnp.cos(phase), amplitude * jnp.sin(phase)], axis=0)


def draw_positions(key, part):
    key_row, key_col = jax.random.split(jax.random.fold_in(key, 202))
    frame = jnp.arange(FRAMES, dtype=jnp.int32)
    owner = frame // F_DEV
    row_tile = owner // COL_TILES
    col_tile = owner % COL_TILES
    row_top = jnp.where(row_tile == ROW_TILES - 1, TR - K + 1, TR).astype(jnp.int32)
    col_top = jnp.where(col_tile == COL_TILES - 1, TC - K + 1, TC).astype(jnp.int32)
    row_off = jax.random.randint(key_row, (FRAMES,), 0, row_top, dtype=jnp.int32)
    col_off = jax.random.randint(key_col, (FRAMES,), 0, col_top, dtype=jnp.int32)
    rows_at = row_tile * TR + row_off
    cols_at = col_tile * TC + col_off
    return jnp.stack([rows_at, cols_at], axis=1).astype(jnp.int32)


def plant(values, own_key, low, top_value):
    index_at = [jax.random.randint(jax.random.fold_in(own_key, axis), (), 0, length) for axis, length in enumerate(values.shape)]
    main_axis = values.shape.index(max(values.shape))
    next_to = index_at[:main_axis] + [(index_at[main_axis] + 1) % values.shape[main_axis]] + index_at[main_axis + 1:]
    return values.at[tuple(index_at)].set(low).at[tuple(next_to)].set(top_value)


def level_of(own_key, dims, cuts, least, largest):
    gain, own = 1.0, jax.random.fold_in(own_key, 6)
    for position, blocks in cuts:
        steps = jnp.exp(jax.random.uniform(jax.random.fold_in(own, position), (blocks,), jnp.float32, least / len(cuts), largest / len(cuts)))
        gain = gain * jnp.repeat(steps, dims[position] // blocks).reshape([-1 if axis == position else 1 for axis in range(len(dims))])
    return gain


def normal_values(own_key, dims, scale, bound, kind=jnp.bfloat16):
    entries = jax.random.normal(own_key, dims, jnp.float32) * scale
    return jnp.minimum(jnp.maximum(entries, -bound), bound).astype(kind)


def setup_inputs(seed: int = 0) -> dict:
    key_of = jax.random.split(jax.random.key(seed), 7)
    object_field = draw_object_field(jax.random.fold_in(key_of[6], 71), 0)
    probe = normal_values(key_of[1], (2, K, K), 0.7, 5.0, jnp.float32)
    kernel_phase = jnp.clip(jax.random.uniform(key_of[2], (K, K), jnp.float32, -3.140625, 3.140625), -3.140625, 3.140625)
    measured = jnp.clip(0.2 + 1.8 * jax.random.uniform(key_of[3], (FRAMES, K, K), jnp.float32) ** level_of(key_of[3], (FRAMES, K, K), ((0, 128),), -0.2, 0.2), 0.2, 2.0)
    positions = draw_positions(jax.random.fold_in(key_of[6], 71), 0)
    batch = plant(jax.random.randint(key_of[5], (FRAMES,), 0, 2), jax.random.fold_in(key_of[5], 1), 0, 1).astype(jnp.int32)
    return {"object_field": object_field, "probe": probe, "kernel_phase": kernel_phase, "measured": measured, "positions": positions, "batch": batch}


def dft_tables(size):
    index = jnp.arange(size, dtype=jnp.int32)
    product = index[:, None] * index[None, :] % size
    angles = product.astype(jnp.float32) * (2.0 * math.pi / size)
    norm_scale = 1.0 / math.sqrt(size)
    return (jnp.cos(angles) * norm_scale, -jnp.sin(angles) * norm_scale)

def matmul_pair(left_real, left_imag, right_real, right_imag):
    first = jnp.matmul(left_real, right_real, precision=lax.Precision.HIGHEST) - jnp.matmul(left_imag, right_imag, precision=lax.Precision.HIGHEST)
    second = jnp.matmul(left_real, right_imag, precision=lax.Precision.HIGHEST) + jnp.matmul(left_imag, right_real, precision=lax.Precision.HIGHEST)
    return (first, second)

def fourier(real_part, imag_part, cos_table, sin_table):
    mid_real, mid_imag = matmul_pair(real_part, imag_part, cos_table, sin_table)
    return matmul_pair(cos_table, sin_table, mid_real, mid_imag)

def frame_pass(patches, probe, kernel, measured, tables):
    cos_table, sin_table = tables
    back_sin = -sin_table
    kernel_real, kernel_imag = kernel
    patch_real = patches[:, 0]
    patch_imag = patches[:, 1]
    layers = patches.shape[2]
    wave_real = probe[0] * patch_real[:, 0] - probe[1] * patch_imag[:, 0]
    wave_imag = probe[0] * patch_imag[:, 0] + probe[1] * patch_real[:, 0]
    incoming = []
    for layer in range(1, layers):
        freq_real, freq_imag = fourier(wave_real, wave_imag, cos_table, sin_table)
        prop_real = freq_real * kernel_real - freq_imag * kernel_imag
        prop_imag = freq_real * kernel_imag + freq_imag * kernel_real
        in_real, in_imag = fourier(prop_real, prop_imag, cos_table, back_sin)
        incoming.append((in_real, in_imag))
        wave_real = patch_real[:, layer] * in_real - patch_imag[:, layer] * in_imag
        wave_imag = patch_real[:, layer] * in_imag + patch_imag[:, layer] * in_real
    far_real, far_imag = fourier(wave_real, wave_imag, cos_table, sin_table)
    power = far_real * far_real + far_imag * far_imag
    factor = 1.0 - measured / jnp.sqrt(jnp.maximum(power, 0.01))
    grad_real, grad_imag = fourier(far_real * factor, far_imag * factor, cos_table, back_sin)
    layer_grads = [None] * layers
    for layer in range(layers - 1, 0, -1):
        in_real, in_imag = incoming[layer - 1]
        layer_grads[layer] = (in_real * grad_real + in_imag * grad_imag, in_real * grad_imag - in_imag * grad_real)
        back_real = patch_real[:, layer] * grad_real + patch_imag[:, layer] * grad_imag
        back_imag = patch_real[:, layer] * grad_imag - patch_imag[:, layer] * grad_real
        freq_real, freq_imag = fourier(back_real, back_imag, cos_table, sin_table)
        conj_real = freq_real * kernel_real + freq_imag * kernel_imag
        conj_imag = freq_imag * kernel_real - freq_real * kernel_imag
        grad_real, grad_imag = fourier(conj_real, conj_imag, cos_table, back_sin)
    layer_grads[0] = (probe[0] * grad_real + probe[1] * grad_imag, probe[0] * grad_imag - probe[1] * grad_real)
    probe_grad = jnp.stack([patch_real[:, 0] * grad_real + patch_imag[:, 0] * grad_imag, patch_real[:, 0] * grad_imag - patch_imag[:, 0] * grad_real], axis=1)
    lighting = patch_real[:, 0] * patch_real[:, 0] + patch_imag[:, 0] * patch_imag[:, 0]
    object_grad = jnp.stack([jnp.stack([item[0] for item in layer_grads], axis=1), jnp.stack([item[1] for item in layer_grads], axis=1)], axis=1)
    return (object_grad, probe_grad, lighting)

def reference(object_field, probe, kernel_phase, measured, positions, batch):
    side = probe.shape[-1]
    layers = object_field.shape[1]
    tables = dft_tables(side)
    kernel = (jnp.cos(kernel_phase), jnp.sin(kernel_phase))
    current = object_field
    beam = probe
    zero = jnp.zeros((), jnp.int32)
    for batch_no in range(BATCHES):

        def visit(carry, frame):
            grads, probe_sum, light_sum = carry
            where, amplitude, which = frame
            starts = (zero, zero, where[0].astype(jnp.int32), where[1].astype(jnp.int32))
            patch = lax.dynamic_slice(current, starts, (2, layers, side, side))
            object_grad, probe_grad, lighting = frame_pass(patch[None], beam, kernel, amplitude[None], tables)
            weight = (which == batch_no).astype(current.dtype)
            piece = lax.dynamic_slice(grads, starts, (2, layers, side, side)) + weight * object_grad[0]
            grads = lax.dynamic_update_slice(grads, piece, starts)
            return ((grads, probe_sum + weight * probe_grad[0], light_sum + weight * lighting[0]), None)
        start_carry = (jnp.zeros_like(current), jnp.zeros_like(beam), jnp.zeros((side, side), beam.dtype))
        (grads, probe_sum, light_sum), _ = lax.scan(visit, start_carry, (positions, measured, batch))
        peak = jnp.max(beam[0] * beam[0] + beam[1] * beam[1])
        current = current - grads / peak
        beam = beam - probe_sum / (light_sum + 1.0)
    return (current, beam)
```

```python
import functools
import math

import jax
import jax.numpy as jnp
import numpy as np
from jax import lax
from jax.experimental import pallas as pl
from jax.experimental.pallas import tpu as pltpu
from jax.sharding import PartitionSpec as P

BATCHES = 2
K = 256
HALF = 128
F32 = jnp.float32
BF16 = jnp.bfloat16


def shifted(value, axis, steps):
    count = lax.axis_size(axis)
    first, last = (max(0, -steps), min(count, count - steps))
    return lax.ppermute(value, axis, [(source, source + steps) for source in range(first, last)])


def packed_total(value, axis):
    return lax.psum(value.reshape(-1), axis).reshape(value.shape)


def bf16_pair(table):
    table = jnp.asarray(table, F32)
    high = table.astype(BF16)
    low = (table - high.astype(F32)).astype(BF16)
    return high, low


def constants():
    index = np.arange(HALF)
    angle = 2.0 * np.pi * (np.outer(index, index) % HALF) / HALF
    cos, sin = np.cos(angle) / 16.0, -np.sin(angle) / 16.0
    right = np.block([[cos, sin], [-sin, cos]])
    right_inv = np.block([[cos, -sin], [sin, cos]])
    rights, lefts = [], []
    for table in (right, right_inv):
        high, low = bf16_pair(table)
        rights.append(jnp.concatenate([high, low, high], axis=0))
        high, low = bf16_pair(table.T)
        lefts.append(jnp.concatenate([high, low, high], axis=1))
    twist = 2.0 * np.pi * index / K
    wr, wi = np.cos(twist).astype(np.float32), -np.sin(twist).astype(np.float32)
    lanes = jnp.asarray(np.stack([np.broadcast_to(wr, (8, HALF)), np.broadcast_to(wi, (8, HALF))]))
    rows = jnp.asarray(np.stack([np.broadcast_to(wr[:, None], (HALF, HALF)), np.broadcast_to(wi[:, None], (HALF, HALF))]))
    return (jnp.stack(rights), jnp.stack(lefts), lanes, rows)


def even_odd(value):
    order = np.concatenate([np.arange(0, K, 2), np.arange(1, K, 2)])
    pick = np.zeros((K, K), np.float32)
    pick[order, np.arange(K)] = 1.0
    pick = jnp.asarray(pick)
    value = jnp.matmul(value, pick, precision=lax.Precision.HIGHEST)
    return jnp.einsum("kn,...kc->...nc", pick, value, precision=lax.Precision.HIGHEST)


def batch_kernel(
    batch_no, at_ref, which_ref, own_ref, right_ref, below_ref, corner_ref, beam_ref, kern_ref, meas_ref,
    mr_ref, ml_ref, wl_ref, wr_ref,
    g_own, g_right, g_below, g_corner, es_ref,
    ext, grad, patch, quantity, urh, url, ulh, ull, vr, vl, sems,
):
    tile = 2 * K
    parts = [
        (own_ref, g_own, pl.ds(0, tile), pl.ds(0, tile)),
        (right_ref, g_right, pl.ds(0, tile), pl.ds(tile, K)),
        (below_ref, g_below, pl.ds(tile, K), pl.ds(0, tile)),
        (corner_ref, g_corner, pl.ds(tile, K), pl.ds(tile, K)),
    ]
    copies = [
        pltpu.make_async_copy(src, ext.at[:, :, rows, cols], sems.at[n]) for n, (src, _, rows, cols) in enumerate(parts)
    ]
    for copy in copies:
        copy.start()
    def clear(i, carry):
        rows = pl.ds(pl.multiple_of(i * 64, 64), 64)
        for c in range(2):
            for layer in range(2):
                grad[c, layer, rows, :] = jnp.zeros((64, 3 * K), F32)
        return carry

    lax.fori_loop(0, 12, clear, 0)
    es_ref[...] = jnp.zeros_like(es_ref)
    for copy in copies:
        copy.wait()

    lane = lax.broadcasted_iota(jnp.int32, (8, HALF), 1)
    sub = lax.broadcasted_iota(jnp.int32, (8, HALF), 0)
    lo, hi = slice(0, HALF), slice(HALF, K)

    def split_to(high_ref, low_ref, rows, cols, value):
        high = value.astype(BF16)
        high_ref[rows, cols] = high
        low_ref[rows, cols] = (value - high.astype(F32)).astype(BF16)

    def dot_right(inverse):
        left = jnp.concatenate([urh[...], urh[...], url[...]], axis=1)
        vr[...] = jnp.dot(left, mr_ref[inverse], preferred_element_type=F32)

    def dot_left(inverse):
        right = jnp.concatenate([ulh[...], ulh[...], ull[...]], axis=0)
        vl[...] = jnp.dot(ml_ref[inverse], right, preferred_element_type=F32)

    def right_in(i, n, ar, ai, br, bi):
        wr, wi = wl_ref[0, 0:1, :], wl_ref[1, 0:1, :]
        dr, di = ar - br, ai - bi
        split_to(urh, url, slice(i, i + n), lo, ar + br)
        split_to(urh, url, slice(i, i + n), hi, ai + bi)
        split_to(urh, url, slice(K + i, K + i + n), lo, dr * wr - di * wi)
        split_to(urh, url, slice(K + i, K + i + n), hi, dr * wi + di * wr)

    def right_out(i, n):
        wr, wi = wl_ref[0, 0:1, :], wl_ref[1, 0:1, :]
        er, ei = vr[i : i + n, lo], vr[i : i + n, hi]
        our, oi = vr[K + i : K + i + n, lo], vr[K + i : K + i + n, hi]
        tr, ti = our * wr + oi * wi, oi * wr - our * wi
        return er + tr, ei + ti, er - tr, ei - ti

    def left_in():
        for i in range(0, HALF, 32):
            wr, wi = wr_ref[0, i : i + 32, :], wr_ref[1, i : i + 32, :]
            for cb in range(2):
                top, low = slice(cb * K + i, cb * K + i + 32), slice(cb * K + HALF + i, cb * K + HALF + i + 32)
                ar, ai, br, bi = vr[top, lo], vr[top, hi], vr[low, lo], vr[low, hi]
                dr, di = ar - br, ai - bi
                even, odd = slice(cb * HALF, cb * HALF + HALF), slice(K + cb * HALF, K + cb * HALF + HALF)
                split_to(ulh, ull, slice(i, i + 32), even, ar + br)
                split_to(ulh, ull, slice(HALF + i, HALF + i + 32), even, ai + bi)
                split_to(ulh, ull, slice(i, i + 32), odd, dr * wr - di * wi)
                split_to(ulh, ull, slice(HALF + i, HALF + i + 32), odd, dr * wi + di * wr)

    def left_out():
        for i in range(0, HALF, 32):
            wr, wi = wr_ref[0, i : i + 32, :], wr_ref[1, i : i + 32, :]
            for cb in range(2):
                even, odd = slice(cb * HALF, cb * HALF + HALF), slice(K + cb * HALF, K + cb * HALF + HALF)
                rr, ii = slice(i, i + 32), slice(HALF + i, HALF + i + 32)
                er, ei, our, oi = vl[rr, even], vl[ii, even], vl[rr, odd], vl[ii, odd]
                tr, ti = our * wr + oi * wi, oi * wr - our * wi
                top, low = slice(cb * K + i, cb * K + i + 32), slice(cb * K + HALF + i, cb * K + HALF + i + 32)
                split_to(urh, url, top, lo, er + tr)
                split_to(urh, url, top, hi, ei + ti)
                split_to(urh, url, low, lo, er - tr)
                split_to(urh, url, low, hi, ei - ti)

    def at_frequency(change):
        for i in range(0, HALF, 32):
            for kb in range(2):
                for cb in range(2):
                    cols = slice(kb * K + cb * HALF, kb * K + cb * HALF + HALF)
                    rr, ii = slice(i, i + 32), slice(HALF + i, HALF + i + 32)
                    at = (slice(kb * HALF + i, kb * HALF + i + 32), slice(cb * HALF, cb * HALF + HALF))
                    re, im = change(vl[rr, cols], vl[ii, cols], at)
                    split_to(ulh, ull, rr, cols, re)
                    split_to(ulh, ull, ii, cols, im)

    def propagate(re, im, at):
        kr, ki = kern_ref[0][at], kern_ref[1][at]
        return re * kr - im * ki, re * ki + im * kr

    def propagate_back(re, im, at):
        kr, ki = kern_ref[0][at], kern_ref[1][at]
        return re * kr + im * ki, im * kr - re * ki

    def frame(f, carry):
        @pl.when(which_ref[f] == batch_no)
        def _():
            row, col = at_ref[f, 0], at_ref[f, 1]
            row_base = pl.multiple_of((row // 8) * 8, 8)
            col_base = pl.multiple_of((col // HALF) * HALF, HALF)
            down, off = row - row_base, col - col_base
            up, back = lax.rem(8 - down, 8), lax.rem(HALF - off, HALF)
            keep, keep_row = lane < HALF - off, sub < 8 - down
            inside, inside_row = lane >= off, sub >= down
            zero = jnp.zeros((8, HALF), F32)

            def window(i, j):
                return pl.ds(pl.multiple_of(row_base + i, 8), 8), pl.ds(pl.multiple_of(col_base + j * HALF, HALF), HALF)

            def cut(step, carry):
                i = step * 32
                for c in range(2):
                    for layer in range(2):
                        columns = []
                        for j in range(3):
                            turned = [
                                pltpu.roll(pltpu.roll(ext[(c, layer) + window(i + 8 * k, j)], back, 1), up, 0) for k in range(5)
                            ]
                            columns.append([jnp.where(keep_row, turned[k], turned[k + 1]) for k in range(4)])
                        for k in range(4):
                            at = pl.ds(pl.multiple_of(i + 8 * k, 8), 8)
                            patch[c, layer, at, lo] = jnp.where(keep, columns[0][k], columns[1][k])
                            patch[c, layer, at, hi] = jnp.where(keep, columns[1][k], columns[2][k])
                return carry

            lax.fori_loop(0, K // 32, cut, 0)

            def place(layer, i, half_r, half_i):
                for c, halves in enumerate((half_r, half_i)):
                    turned = [
                        [pltpu.roll(pltpu.roll(half[8 * k : 8 * k + 8], off, 1), down, 0) for k in range(4)] for half in halves
                    ]
                    left, right = [
                        [
                            jnp.where(inside_row, side[k] if k < 4 else zero, side[k - 1] if k else zero)
                            for k in range(5)
                        ]
                        for side in turned
                    ]
                    for k in range(5):
                        adds = (
                            jnp.where(inside, left[k], zero),
                            jnp.where(inside, right[k], left[k]),
                            jnp.where(inside, zero, right[k]),
                        )
                        for j, add in enumerate(adds):
                            at = (c, layer) + window(i + 8 * k, j)
                            grad[at] = grad[at] + add

            for i in range(0, K, 32):
                rows = slice(i, i + 32)
                waves = []
                for cols in (lo, hi):
                    br, bi = beam_ref[0, rows, cols], beam_ref[1, rows, cols]
                    pr, pi = patch[0, 0, rows, cols], patch[1, 0, rows, cols]
                    waves += [br * pr - bi * pi, br * pi + bi * pr]
                    es_ref[2, rows, cols] = es_ref[2, rows, cols] + (pr * pr + pi * pi)
                right_in(i, 32, *waves)
            dot_right(0)
            left_in()
            dot_left(0)
            at_frequency(propagate)
            dot_left(1)
            left_out()
            dot_right(1)
            for i in range(0, K, 32):
                rows = slice(i, i + 32)
                qs = right_out(i, 32)
                waves = []
                for n, cols in enumerate((lo, hi)):
                    qr, qi = qs[2 * n], qs[2 * n + 1]
                    quantity[0, rows, cols] = qr
                    quantity[1, rows, cols] = qi
                    pr, pi = patch[0, 1, rows, cols], patch[1, 1, rows, cols]
                    waves += [pr * qr - pi * qi, pr * qi + pi * qr]
                right_in(i, 32, *waves)
            dot_right(0)
            left_in()
            dot_left(0)

            def residual(re, im, at):
                power = re * re + im * im
                factor = 1.0 - meas_ref[f, at[0], at[1]] * lax.rsqrt(jnp.maximum(power, 0.01))
                return re * factor, im * factor

            at_frequency(residual)
            dot_left(1)
            left_out()
            dot_right(1)
            for i in range(0, K, 32):
                rows = slice(i, i + 32)
                gs = right_out(i, 32)
                waves, dr, di = [], [], []
                for n, cols in enumerate((lo, hi)):
                    gr, gi = gs[2 * n], gs[2 * n + 1]
                    qr, qi = quantity[0, rows, cols], quantity[1, rows, cols]
                    pr, pi = patch[0, 1, rows, cols], patch[1, 1, rows, cols]
                    dr.append(qr * gr + qi * gi)
                    di.append(qr * gi - qi * gr)
                    waves += [pr * gr + pi * gi, pr * gi - pi * gr]
                right_in(i, 32, *waves)
                place(1, i, dr, di)
            dot_right(0)
            left_in()
            dot_left(0)
            at_frequency(propagate_back)
            dot_left(1)
            left_out()
            dot_right(1)
            for i in range(0, K, 32):
                rows = slice(i, i + 32)
                gs = right_out(i, 32)
                dr, di = [], []
                for n, cols in enumerate((lo, hi)):
                    gr, gi = gs[2 * n], gs[2 * n + 1]
                    br, bi = beam_ref[0, rows, cols], beam_ref[1, rows, cols]
                    pr, pi = patch[0, 0, rows, cols], patch[1, 0, rows, cols]
                    dr.append(br * gr + bi * gi)
                    di.append(br * gi - bi * gr)
                    es_ref[0, rows, cols] = es_ref[0, rows, cols] + (pr * gr + pi * gi)
                    es_ref[1, rows, cols] = es_ref[1, rows, cols] + (pr * gi - pi * gr)
                place(0, i, dr, di)

        return carry

    lax.fori_loop(0, which_ref.shape[0], frame, 0)
    backs = [
        pltpu.make_async_copy(grad.at[:, :, rows, cols], dst, sems.at[n]) for n, (_, dst, rows, cols) in enumerate(parts)
    ]
    for copy in backs:
        copy.start()
    for copy in backs:
        copy.wait()


def run_batch(batch_no, local_at, batch, pieces, beam, kern, meas, tables):
    tile = 2 * K
    smem = pl.BlockSpec(memory_space=pltpu.SMEM)
    vmem = pl.BlockSpec(memory_space=pltpu.VMEM)
    anyw = pl.BlockSpec(memory_space=pl.ANY)
    shapes = [(2, 2, tile, tile), (2, 2, tile, K), (2, 2, K, tile), (2, 2, K, K)]
    return pl.pallas_call(
        functools.partial(batch_kernel, batch_no),
        out_shape=[jax.ShapeDtypeStruct(s, F32) for s in shapes] + [jax.ShapeDtypeStruct((3, K, K), F32)],
        in_specs=[smem, smem] + [anyw] * 4 + [vmem] * 7,
        out_specs=[anyw] * 4 + [vmem],
        scratch_shapes=[
            pltpu.VMEM((2, 2, 3 * K, 3 * K), F32),
            pltpu.VMEM((2, 2, 3 * K, 3 * K), F32),
            pltpu.VMEM((2, 2, K, K), F32),
            pltpu.VMEM((2, K, K), F32),
            pltpu.VMEM((2 * K, K), BF16),
            pltpu.VMEM((2 * K, K), BF16),
            pltpu.VMEM((K, 2 * K), BF16),
            pltpu.VMEM((K, 2 * K), BF16),
            pltpu.VMEM((2 * K, K), F32),
            pltpu.VMEM((K, 2 * K), F32),
            pltpu.SemaphoreType.DMA((4,)),
        ],
        compiler_params=pltpu.CompilerParams(vmem_limit_bytes=48 << 20),
        cost_estimate=pl.CostEstimate(flops=20_000_000_000, bytes_accessed=24 << 20, transcendentals=0),
        name="frames",
    )(local_at, batch, *pieces, beam, kern, meas, *tables)


def shards(object_field, probe, kernel_phase, measured, positions, batch):
    tile = object_field.shape[2]
    tables = constants()
    phase = even_odd(kernel_phase)
    kern = jnp.stack([jnp.cos(phase), jnp.sin(phase)])
    meas = even_odd(measured)
    corner = jnp.stack([lax.axis_index("tile") * tile, lax.axis_index("slab") * tile])
    local_at = positions - corner[None, :].astype(jnp.int32)
    current, beam = object_field, probe
    for batch_no in range(BATCHES):
        right = shifted(current[..., :K], "slab", -1)
        below = shifted(current[:, :, :K, :], "tile", -1)
        diagonal = shifted(right[:, :, :K, :], "tile", -1)
        g_own, g_right, g_below, g_corner, es = run_batch(
            batch_no, local_at, batch, (current, right, below, diagonal), beam, kern, meas, tables
        )
        peak = jnp.max(beam[0] * beam[0] + beam[1] * beam[1])
        from_above = shifted(g_below, "tile", 1)
        right_above = shifted(g_corner, "tile", 1)
        g_right = g_right + jnp.pad(right_above, ((0, 0), (0, 0), (0, tile - K), (0, 0)))
        from_left = shifted(g_right, "slab", 1)
        total = (
            g_own
            + jnp.pad(from_above, ((0, 0), (0, 0), (0, tile - K), (0, 0)))
            + jnp.pad(from_left, ((0, 0), (0, 0), (0, 0), (0, tile - K)))
        )
        current = current - total / peak
        es = packed_total(es, ("tile", "slab"))
        beam = beam - es[:2] / (es[2] + 1.0)
    return (current, beam)


def solution(mesh):
    in_specs = (
        P(None, None, "tile", "slab"),
        P(),
        P(),
        P(("tile", "slab"), None, None),
        P(("tile", "slab"), None),
        P(("tile", "slab")),
    )
    out_specs = (P(None, None, "tile", "slab"), P())
    return jax.shard_map(shards, mesh=mesh, in_specs=in_specs, out_specs=out_specs, check_vma=False)
```

```python
import functools
import math

import jax
import jax.numpy as jnp
import numpy as np
from jax import lax
from jax.experimental import pallas as pl
from jax.experimental.pallas import tpu as pltpu
from jax.sharding import PartitionSpec as P

BATCHES = 2
K = 256
HALF = 128
F32 = jnp.float32
BF16 = jnp.bfloat16


def shifted(value, axis, steps):
    count = lax.axis_size(axis)
    first, last = (max(0, -steps), min(count, count - steps))
    return lax.ppermute(value, axis, [(source, source + steps) for source in range(first, last)])


def bf16_pair(table):
    table = jnp.asarray(table, F32)
    high = table.astype(BF16)
    low = (table - high.astype(F32)).astype(BF16)
    return high, low


def constants():
    index = np.arange(HALF)
    angle = 2.0 * np.pi * (np.outer(index, index) % HALF) / HALF
    cos, sin = np.cos(angle) / 16.0, -np.sin(angle) / 16.0
    right = np.block([[cos, sin], [-sin, cos]])
    right_inv = np.block([[cos, -sin], [sin, cos]])
    rights, lefts = [], []
    for table in (right, right_inv):
        high, low = bf16_pair(table)
        rights.append(jnp.concatenate([high, low, high], axis=0))
        high, low = bf16_pair(table.T)
        lefts.append(jnp.concatenate([high, low, high], axis=1))
    twist = 2.0 * np.pi * index / K
    wr, wi = np.cos(twist).astype(np.float32), -np.sin(twist).astype(np.float32)
    lanes = jnp.asarray(np.stack([np.broadcast_to(wr, (8, HALF)), np.broadcast_to(wi, (8, HALF))]))
    rows = jnp.asarray(np.stack([np.broadcast_to(wr[:, None], (HALF, HALF)), np.broadcast_to(wi[:, None], (HALF, HALF))]))
    return (jnp.stack(rights), jnp.stack(lefts), lanes, rows)


def even_odd(value):
    order = np.concatenate([np.arange(0, K, 2), np.arange(1, K, 2)])
    pick = np.zeros((K, K), np.float32)
    pick[order, np.arange(K)] = 1.0
    pick = jnp.asarray(pick)
    value = jnp.matmul(value, pick, precision=lax.Precision.HIGHEST)
    return jnp.einsum("kn,...kc->...nc", pick, value, precision=lax.Precision.HIGHEST)


def batch_kernel(
    batch_no, at_ref, which_ref, own_ref, right_ref, below_ref, corner_ref, beam_ref, kern_ref, meas_ref,
    mr_ref, ml_ref, wl_ref, wr_ref,
    g_own, g_right, g_below, g_corner, es_ref,
    ext, grad, patch, quantity, urh, url, ulh, ull, vr, vl, sems,
):
    tile = 2 * K
    parts = [
        (own_ref, g_own, pl.ds(0, tile), pl.ds(0, tile)),
        (right_ref, g_right, pl.ds(0, tile), pl.ds(tile, K)),
        (below_ref, g_below, pl.ds(tile, K), pl.ds(0, tile)),
        (corner_ref, g_corner, pl.ds(tile, K), pl.ds(tile, K)),
    ]
    copies = [
        pltpu.make_async_copy(src, ext.at[:, :, rows, cols], sems.at[n]) for n, (src, _, rows, cols) in enumerate(parts)
    ]
    for copy in copies:
        copy.start()
    def clear(i, carry):
        rows = pl.ds(pl.multiple_of(i * 64, 64), 64)
        for c in range(2):
            for layer in range(2):
                grad[c, layer, rows, :] = jnp.zeros((64, 3 * K), F32)
        return carry

    lax.fori_loop(0, 12, clear, 0)
    es_ref[...] = jnp.zeros_like(es_ref)
    for copy in copies:
        copy.wait()

    lane = lax.broadcasted_iota(jnp.int32, (8, HALF), 1)
    sub = lax.broadcasted_iota(jnp.int32, (8, HALF), 0)
    lo, hi = slice(0, HALF), slice(HALF, K)

    def split_to(high_ref, low_ref, rows, cols, value):
        high = value.astype(BF16)
        high_ref[rows, cols] = high
        low_ref[rows, cols] = (value - high.astype(F32)).astype(BF16)

    def dot_right(inverse):
        left = jnp.concatenate([urh[...], urh[...], url[...]], axis=1)
        vr[...] = jnp.dot(left, mr_ref[inverse], preferred_element_type=F32)

    def dot_left(inverse):
        right = jnp.concatenate([ulh[...], ulh[...], ull[...]], axis=0)
        vl[...] = jnp.dot(ml_ref[inverse], right, preferred_element_type=F32)

    def right_in(i, n, ar, ai, br, bi):
        wr, wi = wl_ref[0, 0:1, :], wl_ref[1, 0:1, :]
        dr, di = ar - br, ai - bi
        split_to(urh, url, slice(i, i + n), lo, ar + br)
        split_to(urh, url, slice(i, i + n), hi, ai + bi)
        split_to(urh, url, slice(K + i, K + i + n), lo, dr * wr - di * wi)
        split_to(urh, url, slice(K + i, K + i + n), hi, dr * wi + di * wr)

    def right_out(i, n):
        wr, wi = wl_ref[0, 0:1, :], wl_ref[1, 0:1, :]
        er, ei = vr[i : i + n, lo], vr[i : i + n, hi]
        our, oi = vr[K + i : K + i + n, lo], vr[K + i : K + i + n, hi]
        tr, ti = our * wr + oi * wi, oi * wr - our * wi
        return er + tr, ei + ti, er - tr, ei - ti

    def left_in():
        for i in range(0, HALF, 32):
            wr, wi = wr_ref[0, i : i + 32, :], wr_ref[1, i : i + 32, :]
            for cb in range(2):
                top, low = slice(cb * K + i, cb * K + i + 32), slice(cb * K + HALF + i, cb * K + HALF + i + 32)
                ar, ai, br, bi = vr[top, lo], vr[top, hi], vr[low, lo], vr[low, hi]
                dr, di = ar - br, ai - bi
                even, odd = slice(cb * HALF, cb * HALF + HALF), slice(K + cb * HALF, K + cb * HALF + HALF)
                split_to(ulh, ull, slice(i, i + 32), even, ar + br)
                split_to(ulh, ull, slice(HALF + i, HALF + i + 32), even, ai + bi)
                split_to(ulh, ull, slice(i, i + 32), odd, dr * wr - di * wi)
                split_to(ulh, ull, slice(HALF + i, HALF + i + 32), odd, dr * wi + di * wr)

    def left_out():
        for i in range(0, HALF, 32):
            wr, wi = wr_ref[0, i : i + 32, :], wr_ref[1, i : i + 32, :]
            for cb in range(2):
                even, odd = slice(cb * HALF, cb * HALF + HALF), slice(K + cb * HALF, K + cb * HALF + HALF)
                rr, ii = slice(i, i + 32), slice(HALF + i, HALF + i + 32)
                er, ei, our, oi = vl[rr, even], vl[ii, even], vl[rr, odd], vl[ii, odd]
                tr, ti = our * wr + oi * wi, oi * wr - our * wi
                top, low = slice(cb * K + i, cb * K + i + 32), slice(cb * K + HALF + i, cb * K + HALF + i + 32)
                split_to(urh, url, top, lo, er + tr)
                split_to(urh, url, top, hi, ei + ti)
                split_to(urh, url, low, lo, er - tr)
                split_to(urh, url, low, hi, ei - ti)

    def at_frequency(change):
        for i in range(0, HALF, 32):
            for kb in range(2):
                for cb in range(2):
                    cols = slice(kb * K + cb * HALF, kb * K + cb * HALF + HALF)
                    rr, ii = slice(i, i + 32), slice(HALF + i, HALF + i + 32)
                    at = (slice(kb * HALF + i, kb * HALF + i + 32), slice(cb * HALF, cb * HALF + HALF))
                    re, im = change(vl[rr, cols], vl[ii, cols], at)
                    split_to(ulh, ull, rr, cols, re)
                    split_to(ulh, ull, ii, cols, im)

    def propagate(re, im, at):
        kr, ki = kern_ref[0][at], kern_ref[1][at]
        return re * kr - im * ki, re * ki + im * kr

    def propagate_back(re, im, at):
        kr, ki = kern_ref[0][at], kern_ref[1][at]
        return re * kr + im * ki, im * kr - re * ki

    def frame(f, carry):
        @pl.when(which_ref[f] == batch_no)
        def _():
            row, col = at_ref[f, 0], at_ref[f, 1]
            row_base = pl.multiple_of((row // 8) * 8, 8)
            col_base = pl.multiple_of((col // HALF) * HALF, HALF)
            down, off = row - row_base, col - col_base
            up, back = lax.rem(8 - down, 8), lax.rem(HALF - off, HALF)
            keep, keep_row = lane < HALF - off, sub < 8 - down
            inside, inside_row = lane >= off, sub >= down
            zero = jnp.zeros((8, HALF), F32)

            def window(i, j):
                return pl.ds(pl.multiple_of(row_base + i, 8), 8), pl.ds(pl.multiple_of(col_base + j * HALF, HALF), HALF)

            def cut(step, carry):
                i = step * 32
                for c in range(2):
                    for layer in range(2):
                        columns = []
                        for j in range(3):
                            turned = [
                                pltpu.roll(pltpu.roll(ext[(c, layer) + window(i + 8 * k, j)], back, 1), up, 0) for k in range(5)
                            ]
                            columns.append([jnp.where(keep_row, turned[k], turned[k + 1]) for k in range(4)])
                        for k in range(4):
                            at = pl.ds(pl.multiple_of(i + 8 * k, 8), 8)
                            patch[c, layer, at, lo] = jnp.where(keep, columns[0][k], columns[1][k])
                            patch[c, layer, at, hi] = jnp.where(keep, columns[1][k], columns[2][k])
                return carry

            lax.fori_loop(0, K // 32, cut, 0)

            def place(layer, i, half_r, half_i):
                for c, halves in enumerate((half_r, half_i)):
                    turned = [
                        [pltpu.roll(pltpu.roll(half[8 * k : 8 * k + 8], off, 1), down, 0) for k in range(4)] for half in halves
                    ]
                    left, right = [
                        [
                            jnp.where(inside_row, side[k] if k < 4 else zero, side[k - 1] if k else zero)
                            for k in range(5)
                        ]
                        for side in turned
                    ]
                    for k in range(5):
                        adds = (
                            jnp.where(inside, left[k], zero),
                            jnp.where(inside, right[k], left[k]),
                            jnp.where(inside, zero, right[k]),
                        )
                        for j, add in enumerate(adds):
                            at = (c, layer) + window(i + 8 * k, j)
                            grad[at] = grad[at] + add

            for i in range(0, K, 32):
                rows = slice(i, i + 32)
                waves = []
                for n, cols in enumerate((lo, hi)):
                    br, bi = beam_ref[0, n, rows, :], beam_ref[1, n, rows, :]
                    pr, pi = patch[0, 0, rows, cols], patch[1, 0, rows, cols]
                    waves += [br * pr - bi * pi, br * pi + bi * pr]
                    es_ref[2, n, rows, :] = es_ref[2, n, rows, :] + (pr * pr + pi * pi)
                right_in(i, 32, *waves)
            dot_right(0)
            left_in()
            dot_left(0)
            at_frequency(propagate)
            dot_left(1)
            left_out()
            dot_right(1)
            for i in range(0, K, 32):
                rows = slice(i, i + 32)
                qs = right_out(i, 32)
                waves = []
                for n, cols in enumerate((lo, hi)):
                    qr, qi = qs[2 * n], qs[2 * n + 1]
                    quantity[0, rows, cols] = qr
                    quantity[1, rows, cols] = qi
                    pr, pi = patch[0, 1, rows, cols], patch[1, 1, rows, cols]
                    waves += [pr * qr - pi * qi, pr * qi + pi * qr]
                right_in(i, 32, *waves)
            dot_right(0)
            left_in()
            dot_left(0)

            def residual(re, im, at):
                power = re * re + im * im
                factor = 1.0 - meas_ref[f, at[0], at[1]] * lax.rsqrt(jnp.maximum(power, 0.01))
                return re * factor, im * factor

            at_frequency(residual)
            dot_left(1)
            left_out()
            dot_right(1)
            for i in range(0, K, 32):
                rows = slice(i, i + 32)
                gs = right_out(i, 32)
                waves, dr, di = [], [], []
                for n, cols in enumerate((lo, hi)):
                    gr, gi = gs[2 * n], gs[2 * n + 1]
                    qr, qi = quantity[0, rows, cols], quantity[1, rows, cols]
                    pr, pi = patch[0, 1, rows, cols], patch[1, 1, rows, cols]
                    dr.append(qr * gr + qi * gi)
                    di.append(qr * gi - qi * gr)
                    waves += [pr * gr + pi * gi, pr * gi - pi * gr]
                right_in(i, 32, *waves)
                place(1, i, dr, di)
            dot_right(0)
            left_in()
            dot_left(0)
            at_frequency(propagate_back)
            dot_left(1)
            left_out()
            dot_right(1)
            for i in range(0, K, 32):
                rows = slice(i, i + 32)
                gs = right_out(i, 32)
                dr, di = [], []
                for n, cols in enumerate((lo, hi)):
                    gr, gi = gs[2 * n], gs[2 * n + 1]
                    br, bi = beam_ref[0, n, rows, :], beam_ref[1, n, rows, :]
                    pr, pi = patch[0, 0, rows, cols], patch[1, 0, rows, cols]
                    dr.append(br * gr + bi * gi)
                    di.append(br * gi - bi * gr)
                    es_ref[0, n, rows, :] = es_ref[0, n, rows, :] + (pr * gr + pi * gi)
                    es_ref[1, n, rows, :] = es_ref[1, n, rows, :] + (pr * gi - pi * gr)
                place(0, i, dr, di)

        return carry

    lax.fori_loop(0, which_ref.shape[0], frame, 0)
    backs = [
        pltpu.make_async_copy(grad.at[:, :, rows, cols], dst, sems.at[n]) for n, (_, dst, rows, cols) in enumerate(parts)
    ]
    for copy in backs:
        copy.start()
    for copy in backs:
        copy.wait()


def run_batch(batch_no, local_at, batch, pieces, beam, kern, meas, tables):
    tile = 2 * K
    smem = pl.BlockSpec(memory_space=pltpu.SMEM)
    vmem = pl.BlockSpec(memory_space=pltpu.VMEM)
    anyw = pl.BlockSpec(memory_space=pl.ANY)
    shapes = [(2, 2, tile, tile), (2, 2, tile, K), (2, 2, K, tile), (2, 2, K, K)]
    return pl.pallas_call(
        functools.partial(batch_kernel, batch_no),
        out_shape=[jax.ShapeDtypeStruct(s, F32) for s in shapes] + [jax.ShapeDtypeStruct((3, 2, K, HALF), F32)],
        in_specs=[smem, smem] + [anyw] * 4 + [vmem] * 7,
        out_specs=[anyw] * 4 + [vmem],
        scratch_shapes=[
            pltpu.VMEM((2, 2, 3 * K, 3 * K), F32),
            pltpu.VMEM((2, 2, 3 * K, 3 * K), F32),
            pltpu.VMEM((2, 2, K, K), F32),
            pltpu.VMEM((2, K, K), F32),
            pltpu.VMEM((2 * K, K), BF16),
            pltpu.VMEM((2 * K, K), BF16),
            pltpu.VMEM((K, 2 * K), BF16),
            pltpu.VMEM((K, 2 * K), BF16),
            pltpu.VMEM((2 * K, K), F32),
            pltpu.VMEM((K, 2 * K), F32),
            pltpu.SemaphoreType.DMA((4,)),
        ],
        compiler_params=pltpu.CompilerParams(vmem_limit_bytes=48 << 20),
        cost_estimate=pl.CostEstimate(flops=20_000_000_000, bytes_accessed=24 << 20, transcendentals=0),
        name="frames",
    )(local_at, batch, *pieces, beam, kern, meas, *tables)


MESH = pl.DeviceIdType.MESH
UNITS = 3 * K * K // (8 * HALF)


def exchange_kernel(final, *refs):
    if final:
        es, beam, go, gr, gb, gx, ob = refs[:7]
        beam_new, o_new = refs[7:9]
        rest = refs[9:]
    else:
        es, beam, go, gr, gb, gx, ob, rb = refs[:8]
        beam_new, o_new, r_new, b_new, x_new = refs[8:13]
        rest = refs[13:]
    if final:
        gov, grv, ov, rx, rbl, from_left, tr = rest[:7]
        rest = rest[7:]
    else:
        gov, grv, ov, rx, rbl, from_left, tr, rv, from_right, tl = rest[:10]
        rest = rest[10:]
    scale, rc, acc, rz, acc2, rxs, rys, total, ss, rs, ls = rest
    t, y = lax.axis_index("tile"), lax.axis_index("slab")
    tiles, slabs = 32, 4
    core, x, z = lax.rem(t, 2), lax.rem(t // 2, 4), t // 8
    partner = (t + 1 - 2 * core, y)

    def zpeer(d):
        zp = lax.rem(z + d, 4)
        return zp, ((zp * 4 + x) * 2 + core, y)

    def xpeer(d):
        xp = lax.rem(x + d, 4)
        return xp, ((z * 4 + xp) * 2 + core, y)

    def ypeer(d):
        yp = lax.rem(y + d, 4)
        return yp, (t, yp)

    under, over = (lax.rem(t + 1, tiles), y), (lax.rem(t + tiles - 1, tiles), y)
    rightward, leftward = (t, lax.rem(y + 1, slabs)), (t, lax.rem(y + slabs - 1, slabs))

    sent, used = [], [0]

    def send(src, dst, device):
        n = used[0]
        used[0] += 1
        copy = pltpu.make_async_remote_copy(
            src_ref=src, dst_ref=dst, send_sem=ss.at[n], recv_sem=rs.at[n], device_id=device, device_id_type=MESH
        )
        copy.start()
        sent.append(copy)
        return copy

    local = [pltpu.make_async_copy(go, gov, ls.at[0]), pltpu.make_async_copy(gr, grv, ls.at[1]), pltpu.make_async_copy(ob, ov, ls.at[2])]
    if not final:
        local.append(pltpu.make_async_copy(rb, rv, ls.at[3]))
    for copy in local:
        copy.start()
    barrier = pltpu.get_barrier_semaphore()
    peers = [partner, under, over] + [p(d)[1] for p in (zpeer, xpeer, ypeer) for d in (1, 2, 3)]
    for peer in peers:
        pl.semaphore_signal(barrier, inc=1, device_id=peer, device_id_type=MESH)
    pl.semaphore_wait(barrier, len(peers))

    def reduce_steps():
        half, quarter, part = UNITS // 2, UNITS // 8, UNITS // 32
        copy = send(es.at[pl.ds((1 - core) * half, half)], rc, partner)
        yield
        copy.wait_recv()
        acc[...] = es[pl.ds(core * half, half)] + rc[...]
        copies = []
        for d in (1, 2, 3):
            zp, peer = zpeer(d)
            copies.append(send(acc.at[pl.ds(zp * quarter, quarter)], rz.at[d - 1], peer))
        yield
        for copy in copies:
            copy.wait_recv()
        acc2[...] = acc[pl.ds(z * quarter, quarter)] + (rz[0] + rz[1] + rz[2])
        copies = []
        for d in (1, 2, 3):
            xp, peer = xpeer(d)
            copies.append(send(acc2.at[pl.ds(xp * part, part)], rxs.at[d - 1], peer))
        yield
        for copy in copies:
            copy.wait_recv()
        rys[y] = acc2[pl.ds(x * part, part)] + (rxs[0] + rxs[1] + rxs[2])
        copies = [send(rys.at[y], rys.at[y], ypeer(d)[1]) for d in (1, 2, 3)]
        yield
        for copy in copies:
            copy.wait_recv()
        base = core * half + z * quarter + x * part
        total[pl.ds(base, part)] = (rys[0] + rys[1]) + (rys[2] + rys[3])
        for start, size, targets in (
            (base, part, [xpeer(d)[1] for d in (1, 2, 3)]),
            (core * half + z * quarter, quarter, [zpeer(d)[1] for d in (1, 2, 3)]),
            (core * half, half, [partner]),
        ):
            piece = total.at[pl.ds(start, size)]
            copies = [send(piece, piece, peer) for peer in targets]
            yield
            for copy in copies:
                copy.wait_recv()
        units = UNITS // 3
        for c in range(2):
            at = pl.ds(c * units, units)
            beam_new[at] = beam[at] - total[at] / (total[pl.ds(2 * units, units)] + 1.0)

    top, low = pl.ds(0, K), pl.ds(K, K)
    first, mid = pl.ds(0, K), pl.ds(K, K)

    def sweep(body):
        for layer in range(2):
            def step(i, carry):
                body(layer, i * 32)
                return carry

            lax.fori_loop(0, K // 32, step, 0)

    def rows_at(base, i):
        return pl.ds(pl.multiple_of(base + i, 32), 32)

    def exchange_steps():
        order = (0, 1)
        x_corner, x_mid, y_right, y_left, ups, outs = {}, {}, {}, {}, [], []

        def down(c):
            x_corner[c] = (
                send(gx.at[c], rx.at[c], under),
                send(gb.at[c, :, :, first], rbl.at[c, :, :, first], under),
            )

        def bottom(c):
            y_right[c] = send(gr.at[c, :, low], from_left.at[c, :, low], rightward)
            if not final:
                y_left[c] = send(go.at[c, :, low, first], from_right.at[c, :, low], leftward)

        down(0)
        bottom(0)
        yield
        down(1)
        yield
        bottom(1)
        yield
        for c in order:
            x_mid[c] = send(gb.at[c, :, :, mid], rbl.at[c, :, :, mid], under)
        for copy in local:
            copy.wait()
        units = UNITS // 3
        power = jnp.max(beam[pl.ds(0, units)] ** 2 + beam[pl.ds(units, units)] ** 2, axis=0)
        peak = jnp.max(jnp.max(power, axis=0, keepdims=True), axis=1, keepdims=True)
        scale[...] = jnp.broadcast_to(1.0 / peak, (8, K))
        yield
        y_right_top, y_left_top = {}, {}
        for c in order:
            for copy in x_corner[c]:
                copy.wait_recv()

            def body(layer, i):
                at = rows_at(0, i)
                tr[c, layer, at, :] = grv[c, layer, at, :] + rx[c, layer, at, :]
                if not final:
                    tl[c, layer, at, :] = gov[c, layer, at, first] + rbl[c, layer, at, first]

            sweep(body)
            y_right_top[c] = send(tr.at[c], from_left.at[c, :, top], rightward)
            if not final:
                y_left_top[c] = send(tl.at[c], from_right.at[c, :, top], leftward)
            yield
        for c in order:
            x_mid[c].wait_recv()

            def body(layer, i):
                at, inv = rows_at(0, i), scale[0:1, :]
                ov[c, layer, at, mid] = ov[c, layer, at, mid] - (gov[c, layer, at, mid] + rbl[c, layer, at, mid]) * inv
                at = rows_at(K, i)
                ov[c, layer, at, mid] = ov[c, layer, at, mid] - gov[c, layer, at, mid] * inv

            sweep(body)
            if not final:
                ups.append(send(ov.at[c, :, top, mid], b_new.at[c, :, :, mid], over))
            yield
        for c in order:
            y_right[c].wait_recv()
            if not final:
                y_left[c].wait_recv()

            def body(layer, i):
                at, inv = rows_at(K, i), scale[0:1, :]
                ov[c, layer, at, first] = ov[c, layer, at, first] - (gov[c, layer, at, first] + from_left[c, layer, at, :]) * inv
                if not final:
                    rv[c, layer, at, :] = rv[c, layer, at, :] - (grv[c, layer, at, :] + from_right[c, layer, at, :]) * inv

            sweep(body)
            yield
        for c in order:
            y_right_top[c].wait_recv()
            if not final:
                y_left_top[c].wait_recv()

            def body(layer, i):
                at, inv = rows_at(0, i), scale[0:1, :]
                if final:
                    own = gov[c, layer, at, first] + rbl[c, layer, at, first]
                else:
                    own = tl[c, layer, at, :]
                    rv[c, layer, at, :] = rv[c, layer, at, :] - (tr[c, layer, at, :] + from_right[c, layer, at, :]) * inv
                ov[c, layer, at, first] = ov[c, layer, at, first] - (own + from_left[c, layer, at, :]) * inv

            sweep(body)
            if not final:
                ups.append(send(ov.at[c, :, top, first], b_new.at[c, :, :, first], over))
                ups.append(send(rv.at[c, :, top], x_new.at[c], over))
            outs.append(pltpu.make_async_copy(ov.at[c], o_new.at[c], ls.at[4 + 2 * c]))
            if not final:
                outs.append(pltpu.make_async_copy(rv.at[c], r_new.at[c], ls.at[5 + 2 * c]))
            for copy in outs[-1 if final else -2 :]:
                copy.start()
            yield
        for copy in ups:
            copy.wait_recv()
        for copy in outs:
            copy.wait()

    reduce_run, exchange_run = reduce_steps(), exchange_steps()
    for turn in "rerrererrereerereeee":
        next(reduce_run if turn == "r" else exchange_run, None)
    for run in (exchange_run, reduce_run):
        for _ in run:
            pass
    for copy in sent:
        copy.wait_send()


def run_exchange(final, es, beam, grads, own, right):
    tile = 2 * K
    vmem = pl.BlockSpec(memory_space=pltpu.VMEM)
    anyw = pl.BlockSpec(memory_space=pl.ANY)
    shape = jax.ShapeDtypeStruct
    square, strip = pltpu.VMEM((2, 2, tile, tile), F32), pltpu.VMEM((2, 2, tile, K), F32)
    flat, small = pltpu.VMEM((2, 2, K, tile), F32), pltpu.VMEM((2, 2, K, K), F32)
    scratch = [square, strip, square, small, flat, strip, small] + ([] if final else [strip, strip, small])
    scratch += [
        pltpu.VMEM((8, K), F32),
        pltpu.VMEM((UNITS // 2, 8, HALF), F32),
        pltpu.VMEM((UNITS // 2, 8, HALF), F32),
        pltpu.VMEM((3, UNITS // 8, 8, HALF), F32),
        pltpu.VMEM((UNITS // 8, 8, HALF), F32),
        pltpu.VMEM((3, UNITS // 32, 8, HALF), F32),
        pltpu.VMEM((4, UNITS // 32, 8, HALF), F32),
        pltpu.VMEM((UNITS, 8, HALF), F32),
        pltpu.SemaphoreType.DMA((48,)),
        pltpu.SemaphoreType.DMA((48,)),
        pltpu.SemaphoreType.DMA((8,)),
    ]
    outs = [shape(beam.shape, F32), shape((2, 2, tile, tile), F32)]
    operands = [es, beam, *grads, own]
    if not final:
        outs += [shape((2, 2, tile, K), F32), shape((2, 2, K, tile), F32), shape((2, 2, K, K), F32)]
        operands.append(right)
    return pl.pallas_call(
        functools.partial(exchange_kernel, final),
        out_shape=outs,
        in_specs=[vmem, vmem] + [anyw] * (len(operands) - 2),
        out_specs=[vmem] + [anyw] * (len(outs) - 1),
        scratch_shapes=scratch,
        compiler_params=pltpu.CompilerParams(
            collective_id=1 if final else 0, has_side_effects=True, vmem_limit_bytes=48 << 20
        ),
        name="close" if final else "exchange",
    )(*operands)


def shards(object_field, probe, kernel_phase, measured, positions, batch):
    tile = object_field.shape[2]
    tables = constants()
    phase = even_odd(kernel_phase)
    kern = jnp.stack([jnp.cos(phase), jnp.sin(phase)])
    meas = even_odd(measured)
    corner = jnp.stack([lax.axis_index("tile") * tile, lax.axis_index("slab") * tile])
    local_at = positions - corner[None, :].astype(jnp.int32)
    beam = probe.reshape(2, K, 2, HALF).transpose(0, 2, 1, 3)
    own = object_field
    right = shifted(own[..., :K], "slab", -1)
    below = shifted(own[:, :, :K, :], "tile", -1)
    diagonal = shifted(right[:, :, :K, :], "tile", -1)
    for batch_no in range(BATCHES):
        *grads, es = run_batch(batch_no, local_at, batch, (own, right, below, diagonal), beam, kern, meas, tables)
        flat = beam.reshape(UNITS * 2 // 3, 8, HALF)
        es = es.reshape(UNITS, 8, HALF)
        if batch_no + 1 < BATCHES:
            flat, own, right, below, diagonal = run_exchange(False, es, flat, grads, own, right)
        else:
            flat, own = run_exchange(True, es, flat, grads, own, None)
        beam = flat.reshape(2, 2, K, HALF)
    return (own, beam.transpose(0, 2, 1, 3).reshape(2, K, K))


def solution(mesh):
    in_specs = (
        P(None, None, "tile", "slab"),
        P(),
        P(),
        P(("tile", "slab"), None, None),
        P(("tile", "slab"), None),
        P(("tile", "slab")),
    )
    out_specs = (P(None, None, "tile", "slab"), P())
    return jax.shard_map(shards, mesh=mesh, in_specs=in_specs, out_specs=out_specs, check_vma=False)
```

```python
import functools
import math

import jax
import jax.numpy as jnp
import numpy as np
from jax import lax
from jax.experimental import pallas as pl
from jax.experimental.pallas import tpu as pltpu
from jax.sharding import PartitionSpec as P

BATCHES = 2
K = 256
HALF = 128
F32 = jnp.float32
BF16 = jnp.bfloat16


def bf16_pair(table):
    table = jnp.asarray(table, F32)
    high = table.astype(BF16)
    low = (table - high.astype(F32)).astype(BF16)
    return high, low


def constants():
    index = np.arange(HALF)
    angle = 2.0 * np.pi * (np.outer(index, index) % HALF) / HALF
    cos, sin = np.cos(angle) / 16.0, -np.sin(angle) / 16.0
    right = np.block([[cos, sin], [-sin, cos]])
    right_inv = np.block([[cos, -sin], [sin, cos]])
    rights, lefts = [], []
    for table in (right, right_inv):
        high, low = bf16_pair(table)
        rights.append(jnp.concatenate([high, low, high], axis=0))
        high, low = bf16_pair(table.T)
        lefts.append(jnp.concatenate([high, low, high], axis=1))
    twist = 2.0 * np.pi * index / K
    wr, wi = np.cos(twist).astype(np.float32), -np.sin(twist).astype(np.float32)
    lanes = jnp.asarray(np.stack([np.broadcast_to(wr, (8, HALF)), np.broadcast_to(wi, (8, HALF))]))
    rows = jnp.asarray(np.stack([np.broadcast_to(wr[:, None], (HALF, HALF)), np.broadcast_to(wi[:, None], (HALF, HALF))]))
    return (jnp.stack(rights), jnp.stack(lefts), lanes, rows)


def even_odd(value):
    order = np.concatenate([np.arange(0, K, 2), np.arange(1, K, 2)])
    pick = np.zeros((K, K), np.float32)
    pick[order, np.arange(K)] = 1.0
    pick = jnp.asarray(pick)
    value = jnp.matmul(value, pick, precision=lax.Precision.HIGHEST)
    return jnp.einsum("kn,...kc->...nc", pick, value, precision=lax.Precision.HIGHEST)


def batch_kernel(
    batch_no, at_ref, which_ref, ext, beam_ref, kern_ref, meas_hbm, mr_ref, ml_ref, wl_ref, wr_ref,
    g_out, es_ref,
    grad, window, meas_ref, patch, quantity, vr, vl, chosen, sems,
):
    count = jnp.int32(0)
    for f in range(which_ref.shape[0]):
        mine = which_ref[f] == batch_no

        @pl.when(mine)
        def _():
            chosen[count] = f

        count = count + mine.astype(jnp.int32)

    def corner_of(f):
        row, col = at_ref[f, 0], at_ref[f, 1]
        return pl.multiple_of((row // 8) * 8, 8), pl.multiple_of((col // HALF) * HALF, HALF)

    def fetches(n):
        f, slot = chosen[n], lax.rem(n, 2)
        row_base, col_base = corner_of(f)
        return (
            pltpu.make_async_copy(
                ext.at[:, :, pl.ds(row_base, K + 8), pl.ds(col_base, K + HALF)], window.at[slot], sems.at[slot]
            ),
            pltpu.make_async_copy(meas_hbm.at[f], meas_ref.at[slot], sems.at[2 + slot]),
        )

    def fetch(n):
        @pl.when(n < count)
        def _():
            for copy in fetches(n):
                copy.start()

    fetch(jnp.int32(0))

    def returns(layer):
        return [pltpu.make_async_copy(grad.at[c, layer], g_out.at[c, layer], sems.at[4 + 2 * c + layer]) for c in range(2)]

    def clear(i, carry):
        rows = pl.ds(pl.multiple_of(i * 64, 64), 64)
        for c in range(2):
            for layer in range(2):
                grad[c, layer, rows, :] = jnp.zeros((64, 3 * K), F32)
        return carry

    lax.fori_loop(0, 12, clear, 0)
    es_ref[...] = jnp.zeros_like(es_ref)

    lane = lax.broadcasted_iota(jnp.int32, (8, HALF), 1)
    sub = lax.broadcasted_iota(jnp.int32, (8, HALF), 0)
    lo, hi = slice(0, HALF), slice(HALF, K)

    def operand(blocks):
        highs = [[block.astype(BF16) for block in row] for row in blocks]
        lows = [
            [(block - high.astype(F32)).astype(BF16) for block, high in zip(row, parts)] for row, parts in zip(blocks, highs)
        ]
        return [jnp.concatenate([jnp.concatenate(row, axis=1) for row in rows], axis=0) for rows in (highs, lows)]

    def dot_right(inverse, cb, blocks):
        high, low = operand(blocks)
        vr[cb] = jnp.dot(jnp.concatenate([high, high, low], axis=1), mr_ref[inverse], preferred_element_type=F32)

    def dot_left(inverse, cb, blocks):
        high, low = operand(blocks)
        vl[cb] = jnp.dot(ml_ref[inverse], jnp.concatenate([high, high, low], axis=0), preferred_element_type=F32)

    def right_in(ar, ai, br, bi):
        wr, wi = wl_ref[0, 0:1, :], wl_ref[1, 0:1, :]
        dr, di = ar - br, ai - bi
        return [ar + br, ai + bi], [dr * wr - di * wi, dr * wi + di * wr]

    def right_out(i, n):
        wr, wi = wl_ref[0, 0:1, :], wl_ref[1, 0:1, :]
        rows = slice(i, i + n)
        er, ei, our, oi = vr[0, rows, lo], vr[0, rows, hi], vr[1, rows, lo], vr[1, rows, hi]
        tr, ti = our * wr + oi * wi, oi * wr - our * wi
        return er + tr, ei + ti, er - tr, ei - ti

    def left_in(cb):
        tops, lows = [], []
        for i in range(0, HALF, 32):
            wr, wi = wr_ref[0, i : i + 32, :], wr_ref[1, i : i + 32, :]
            top, low = slice(i, i + 32), slice(HALF + i, HALF + i + 32)
            ar, ai, br, bi = vr[cb, top, lo], vr[cb, top, hi], vr[cb, low, lo], vr[cb, low, hi]
            dr, di = ar - br, ai - bi
            tops.append([ar + br, dr * wr - di * wi])
            lows.append([ai + bi, dr * wi + di * wr])
        return tops + lows

    def left_out(cb):
        tops, lows = [], []
        for i in range(0, HALF, 32):
            wr, wi = wr_ref[0, i : i + 32, :], wr_ref[1, i : i + 32, :]
            top, low = slice(i, i + 32), slice(HALF + i, HALF + i + 32)
            er, ei, our, oi = vl[cb, top, lo], vl[cb, low, lo], vl[cb, top, hi], vl[cb, low, hi]
            tr, ti = our * wr + oi * wi, oi * wr - our * wi
            tops.append([er + tr, ei + ti])
            lows.append([er - tr, ei - ti])
        return tops + lows

    def at_frequency(change, cb):
        tops, lows = [], []
        for i in range(0, HALF, 32):
            pair = []
            for kb, cols in enumerate((lo, hi)):
                top, low = slice(i, i + 32), slice(HALF + i, HALF + i + 32)
                at = (slice(kb * HALF + i, kb * HALF + i + 32), slice(cb * HALF, cb * HALF + HALF))
                pair.append(change(vl[cb, top, cols], vl[cb, low, cols], at))
            tops.append([pair[0][0], pair[1][0]])
            lows.append([pair[0][1], pair[1][1]])
        return tops + lows

    def both_ways(change, evens, odds):
        dot_right(0, 0, evens)
        dot_right(0, 1, odds)
        for cb in range(2):
            dot_left(0, cb, left_in(cb))
        for cb in range(2):
            dot_left(1, cb, at_frequency(change, cb))
        for cb in range(2):
            dot_right(1, cb, left_out(cb))

    def propagate(re, im, at):
        kr, ki = kern_ref[0][at], kern_ref[1][at]
        return re * kr - im * ki, re * ki + im * kr

    def propagate_back(re, im, at):
        kr, ki = kern_ref[0][at], kern_ref[1][at]
        return re * kr + im * ki, im * kr - re * ki

    def frame(n, carry):
        if n is not None:
            f, slot = chosen[n], lax.rem(n, 2)
            fetch(n + 1)
            for copy in fetches(n):
                copy.wait()
            row, col = at_ref[f, 0], at_ref[f, 1]
            row_base, col_base = corner_of(f)
            down, off = row - row_base, col - col_base
            up, back = lax.rem(8 - down, 8), lax.rem(HALF - off, HALF)
            keep, keep_row = lane < HALF - off, sub < 8 - down
            inside, inside_row = lane >= off, sub >= down
            zero = jnp.zeros((8, HALF), F32)

            def target(i, j):
                return pl.ds(pl.multiple_of(row_base + i, 8), 8), pl.ds(pl.multiple_of(col_base + j * HALF, HALF), HALF)

            def cut(step, carry):
                i = step * 32
                for c in range(2):
                    for layer in range(2):
                        columns = []
                        for j in range(3):
                            turned = [
                                pltpu.roll(
                                    pltpu.roll(
                                        window[slot, c, layer, pl.ds(pl.multiple_of(i + 8 * k, 8), 8), HALF * j : HALF * (j + 1)],
                                        back, 1,
                                    ),
                                    up, 0,
                                )
                                for k in range(5)
                            ]
                            columns.append([jnp.where(keep_row, turned[k], turned[k + 1]) for k in range(4)])
                        for k in range(4):
                            at = pl.ds(pl.multiple_of(i + 8 * k, 8), 8)
                            patch[c, layer, at, lo] = jnp.where(keep, columns[0][k], columns[1][k])
                            patch[c, layer, at, hi] = jnp.where(keep, columns[1][k], columns[2][k])
                return carry

            lax.fori_loop(0, K // 32, cut, 0)

            def place(layer, i, half_r, half_i):
                for c, halves in enumerate((half_r, half_i)):
                    turned = [
                        [pltpu.roll(pltpu.roll(half[8 * k : 8 * k + 8], off, 1), down, 0) for k in range(4)] for half in halves
                    ]
                    left, right = [
                        [
                            jnp.where(inside_row, side[k] if k < 4 else zero, side[k - 1] if k else zero)
                            for k in range(5)
                        ]
                        for side in turned
                    ]
                    for k in range(5):
                        adds = (
                            jnp.where(inside, left[k], zero),
                            jnp.where(inside, right[k], left[k]),
                            jnp.where(inside, zero, right[k]),
                        )
                        for j, add in enumerate(adds):
                            at = (c, layer) + target(i + 8 * k, j)
                            grad[at] = grad[at] + add

            evens, odds = [], []
            for i in range(0, K, 32):
                rows = slice(i, i + 32)
                waves = []
                for n, cols in enumerate((lo, hi)):
                    br, bi = beam_ref[0, n, rows, :], beam_ref[1, n, rows, :]
                    pr, pi = patch[0, 0, rows, cols], patch[1, 0, rows, cols]
                    waves += [br * pr - bi * pi, br * pi + bi * pr]
                    es_ref[2, n, rows, :] = es_ref[2, n, rows, :] + (pr * pr + pi * pi)
                even, odd = right_in(*waves)
                evens.append(even)
                odds.append(odd)
            both_ways(propagate, evens, odds)
            evens, odds = [], []
            for i in range(0, K, 32):
                rows = slice(i, i + 32)
                qs = right_out(i, 32)
                waves = []
                for n, cols in enumerate((lo, hi)):
                    qr, qi = qs[2 * n], qs[2 * n + 1]
                    quantity[0, rows, cols] = qr
                    quantity[1, rows, cols] = qi
                    pr, pi = patch[0, 1, rows, cols], patch[1, 1, rows, cols]
                    waves += [pr * qr - pi * qi, pr * qi + pi * qr]
                even, odd = right_in(*waves)
                evens.append(even)
                odds.append(odd)
            def residual(re, im, at):
                power = re * re + im * im
                factor = 1.0 - meas_ref[slot, at[0], at[1]] * lax.rsqrt(jnp.maximum(power, 0.01))
                return re * factor, im * factor

            both_ways(residual, evens, odds)
            evens, odds = [], []
            for i in range(0, K, 32):
                rows = slice(i, i + 32)
                gs = right_out(i, 32)
                waves, dr, di = [], [], []
                for n, cols in enumerate((lo, hi)):
                    gr, gi = gs[2 * n], gs[2 * n + 1]
                    qr, qi = quantity[0, rows, cols], quantity[1, rows, cols]
                    pr, pi = patch[0, 1, rows, cols], patch[1, 1, rows, cols]
                    dr.append(qr * gr + qi * gi)
                    di.append(qr * gi - qi * gr)
                    waves += [pr * gr + pi * gi, pr * gi - pi * gr]
                even, odd = right_in(*waves)
                evens.append(even)
                odds.append(odd)
                place(1, i, dr, di)

            both_ways(propagate_back, evens, odds)
            evens, odds = [], []
            for i in range(0, K, 32):
                rows = slice(i, i + 32)
                gs = right_out(i, 32)
                dr, di = [], []
                for n, cols in enumerate((lo, hi)):
                    gr, gi = gs[2 * n], gs[2 * n + 1]
                    br, bi = beam_ref[0, n, rows, :], beam_ref[1, n, rows, :]
                    pr, pi = patch[0, 0, rows, cols], patch[1, 0, rows, cols]
                    dr.append(br * gr + bi * gi)
                    di.append(br * gi - bi * gr)
                    es_ref[0, n, rows, :] = es_ref[0, n, rows, :] + (pr * gr + pi * gi)
                    es_ref[1, n, rows, :] = es_ref[1, n, rows, :] + (pr * gi - pi * gr)
                place(0, i, dr, di)

        return carry

    lax.fori_loop(0, count, frame, 0)

    for copy in returns(0) + returns(1):
        copy.start()
    for copy in returns(0) + returns(1):
        copy.wait()


def run_batch(batch_no, local_at, batch, ext, beam, kern, meas, tables):
    smem = pl.BlockSpec(memory_space=pltpu.SMEM)
    vmem = pl.BlockSpec(memory_space=pltpu.VMEM)
    anyw = pl.BlockSpec(memory_space=pl.ANY)
    return pl.pallas_call(
        functools.partial(batch_kernel, batch_no),
        out_shape=[jax.ShapeDtypeStruct((2, 2, 3 * K, 3 * K), F32), jax.ShapeDtypeStruct((3, 2, K, HALF), F32)],
        in_specs=[smem, smem, anyw, vmem, vmem, anyw] + [vmem] * 4,
        out_specs=[anyw, vmem],
        scratch_shapes=[
            pltpu.VMEM((2, 2, 3 * K, 3 * K), F32),
            pltpu.VMEM((2, 2, 2, K + 8, K + HALF), F32),
            pltpu.VMEM((2, K, K), F32),
            pltpu.VMEM((2, 2, K, K), F32),
            pltpu.VMEM((2, K, K), F32),
            pltpu.VMEM((2, K, K), F32),
            pltpu.VMEM((2, K, K), F32),
            pltpu.SMEM((4,), jnp.int32),
            pltpu.SemaphoreType.DMA((8,)),
        ],
        compiler_params=pltpu.CompilerParams(vmem_limit_bytes=48 << 20),
        cost_estimate=pl.CostEstimate(flops=20_000_000_000, bytes_accessed=24 << 20, transcendentals=0),
        name="frames",
    )(local_at, batch, ext, beam, kern, meas, *tables)


MESH = pl.DeviceIdType.MESH
UNITS = 3 * K * K // (8 * HALF)


ORDER = {
    False: "rbrrdbrdbrdbLdtrmttrtmmmMrMMMBBBBTTTTU",
    True: "rdbbrdrbbdLrttdrmmttmrmMrMBrMMBBBTTTTU",
}
PLANES = [(0, 0), (1, 0), (0, 1), (1, 1)]


class Net:
    def __init__(self, send_sems, recv_sems):
        self.t, self.y = t, y = lax.axis_index("tile"), lax.axis_index("slab")
        self.core, self.x, self.z = lax.rem(t, 2), lax.rem(t // 2, 4), t // 8
        self.partner = (t + 1 - 2 * self.core, y)
        self.under, self.over = (lax.rem(t + 1, 32), y), (lax.rem(t + 31, 32), y)
        self.rightward, self.leftward = (t, lax.rem(y + 1, 4)), (t, lax.rem(y + 3, 4))
        self.sems, self.sent = (send_sems, recv_sems), []

    def send(self, src, dst, device):
        n = len(self.sent)
        copy = pltpu.make_async_remote_copy(
            src_ref=src, dst_ref=dst, send_sem=self.sems[0].at[n], recv_sem=self.sems[1].at[n],
            device_id=device, device_id_type=MESH,
        )
        copy.start()
        self.sent.append(copy)
        return copy

    def meet(self, peers):
        barrier = pltpu.get_barrier_semaphore()
        for peer in peers:
            pl.semaphore_signal(barrier, inc=1, device_id=peer, device_id_type=MESH)
        pl.semaphore_wait(barrier, len(peers))

    def finish(self):
        for copy in self.sent:
            copy.wait_send()


def open_kernel(own, ext, held, ss, rs, ls):
    net = Net(ss, rs)
    inward = [pltpu.make_async_copy(own.at[c, layer], held.at[c, layer], ls.at[2 * c + layer]) for c, layer in PLANES]
    for copy in inward:
        copy.start()
    net.meet([net.over, net.under, net.leftward, net.rightward])
    top, low, first = pl.ds(0, K), pl.ds(K, K), pl.ds(0, K)
    outer = pl.ds(2 * K, K)
    tops = [net.send(own.at[p + (top, first)], ext.at[p + (top, outer)], net.leftward) for p in PLANES]
    belows = [net.send(own.at[p + (top,)], ext.at[p + (outer, pl.ds(0, 2 * K))], net.over) for p in PLANES]
    lows = [net.send(own.at[p + (low, first)], ext.at[p + (low, outer)], net.leftward) for p in PLANES]
    for copy in inward:
        copy.wait()
    outward = [
        pltpu.make_async_copy(held.at[p], ext.at[p + (pl.ds(0, 2 * K), pl.ds(0, 2 * K))], ls.at[2 * p[0] + p[1]]) for p in PLANES
    ]
    for copy in outward:
        copy.start()
    corners = []
    for p, copy in zip(PLANES, tops):
        copy.wait_recv()
        corners.append(net.send(ext.at[p + (top, outer)], ext.at[p + (outer, outer)], net.over))
    for copy in belows + lows + corners:
        copy.wait_recv()
    for copy in outward:
        copy.wait()
    net.finish()


def run_open(own):
    anyw = pl.BlockSpec(memory_space=pl.ANY)
    return pl.pallas_call(
        open_kernel,
        out_shape=jax.ShapeDtypeStruct((2, 2, 3 * K, 3 * K), F32),
        in_specs=[anyw],
        out_specs=anyw,
        scratch_shapes=[
            pltpu.VMEM((2, 2, 2 * K, 2 * K), F32),
            pltpu.SemaphoreType.DMA((16,)),
            pltpu.SemaphoreType.DMA((16,)),
            pltpu.SemaphoreType.DMA((4,)),
        ],
        compiler_params=pltpu.CompilerParams(collective_id=2, has_side_effects=True, vmem_limit_bytes=48 << 20),
        name="open",
    )(own)


def exchange_kernel(final, *refs):
    es, beam, g, ext, beam_new, new = refs[:6]
    gov, grv, ov, rx, rbl, from_left, tr = refs[6:13]
    rest = refs[13:]
    if not final:
        rv, from_right, tl = rest[:3]
        rest = rest[3:]
    scale, rc, acc, rz, acc2, rxs, rys, total, ss, rs, ls = rest
    net = Net(ss, rs)
    core, x, y, z, partner, send = net.core, net.x, net.y, net.z, net.partner, net.send
    under, over, rightward, leftward = net.under, net.over, net.rightward, net.leftward

    def zpeer(d):
        zp = lax.rem(z + d, 4)
        return zp, ((zp * 4 + x) * 2 + core, y)

    def xpeer(d):
        xp = lax.rem(x + d, 4)
        return xp, ((z * 4 + xp) * 2 + core, y)

    def ypeer(d):
        yp = lax.rem(y + d, 4)
        return yp, (net.t, yp)

    whole, outer = pl.ds(0, 2 * K), pl.ds(2 * K, K)
    square, strip = (slice(None), slice(None), whole, whole), (slice(None), slice(None), whole, outer)
    local = [
        pltpu.make_async_copy(g.at[square], gov, ls.at[0]),
        pltpu.make_async_copy(g.at[strip], grv, ls.at[1]),
        pltpu.make_async_copy(ext.at[square], ov, ls.at[2]),
    ]
    if not final:
        local.append(pltpu.make_async_copy(ext.at[strip], rv, ls.at[3]))
    for copy in local:
        copy.start()
    net.meet([partner, under, over] + [p(d)[1] for p in (zpeer, xpeer, ypeer) for d in (1, 2, 3)])

    def reduce_steps():
        half, quarter, part = UNITS // 2, UNITS // 8, UNITS // 32
        copy = send(es.at[pl.ds((1 - core) * half, half)], rc, partner)
        yield
        copy.wait_recv()
        acc[...] = es[pl.ds(core * half, half)] + rc[...]
        copies = []
        for d in (1, 2, 3):
            zp, peer = zpeer(d)
            copies.append(send(acc.at[pl.ds(zp * quarter, quarter)], rz.at[d - 1], peer))
        yield
        for copy in copies:
            copy.wait_recv()
        acc2[...] = acc[pl.ds(z * quarter, quarter)] + (rz[0] + rz[1] + rz[2])
        copies = []
        for d in (1, 2, 3):
            xp, peer = xpeer(d)
            copies.append(send(acc2.at[pl.ds(xp * part, part)], rxs.at[d - 1], peer))
        yield
        for copy in copies:
            copy.wait_recv()
        rys[y] = acc2[pl.ds(x * part, part)] + (rxs[0] + rxs[1] + rxs[2])
        copies = [send(rys.at[y], rys.at[y], ypeer(d)[1]) for d in (1, 2, 3)]
        yield
        for copy in copies:
            copy.wait_recv()
        base = core * half + z * quarter + x * part
        total[pl.ds(base, part)] = (rys[0] + rys[1]) + (rys[2] + rys[3])
        for start, size, targets in (
            (base, part, [xpeer(d)[1] for d in (1, 2, 3)]),
            (core * half + z * quarter, quarter, [zpeer(d)[1] for d in (1, 2, 3)]),
            (core * half, half, [partner]),
        ):
            piece = total.at[pl.ds(start, size)]
            copies = [send(piece, piece, peer) for peer in targets]
            yield
            for copy in copies:
                copy.wait_recv()
        units = UNITS // 3
        for c in range(2):
            at = pl.ds(c * units, units)
            beam_new[at] = beam[at] - total[at] / (total[pl.ds(2 * units, units)] + 1.0)

    top, low = pl.ds(0, K), pl.ds(K, K)
    first, mid = pl.ds(0, K), pl.ds(K, K)

    def sweep(body):
        def step(i, carry):
            body(i * 32)
            return carry

        lax.fori_loop(0, K // 32, step, 0)

    def rows_at(base, i):
        return pl.ds(pl.multiple_of(base + i, 32), 32)

    corners, mids, lows, tops, ups, outs = {}, {}, {}, {}, [], []

    def down(p):
        corners[p] = (
            send(g.at[p + (outer, outer)], rx.at[p], under),
            send(g.at[p + (outer, first)], rbl.at[p + (slice(None), first)], under),
        )

    def bottom(p):
        lows[p] = [send(g.at[p + (low, outer)], from_left.at[p + (low,)], rightward)]
        if not final:
            lows[p].append(send(g.at[p + (low, first)], from_right.at[p + (low,)], leftward))

    def middle(p):
        mids[p] = send(g.at[p + (outer, mid)], rbl.at[p + (slice(None), mid)], under)

    def ready(_):
        for copy in local:
            copy.wait()
        units = UNITS // 3
        power = jnp.max(beam[pl.ds(0, units)] ** 2 + beam[pl.ds(units, units)] ** 2, axis=0)
        peak = jnp.max(jnp.max(power, axis=0, keepdims=True), axis=1, keepdims=True)
        scale[...] = jnp.broadcast_to(1.0 / peak, (8, K))

    def send_top(p):
        for copy in corners[p]:
            copy.wait_recv()

        def body(i):
            at = p + (rows_at(0, i),)
            tr[at] = grv[at] + rx[at]
            if not final:
                tl[at] = gov[at + (first,)] + rbl[at + (first,)]

        sweep(body)
        tops[p] = [send(tr.at[p], from_left.at[p + (top,)], rightward)]
        if not final:
            tops[p].append(send(tl.at[p], from_right.at[p + (top,)], leftward))

    def use_middle(p):
        mids[p].wait_recv()

        def body(i):
            inv = scale[0:1, :]
            at = p + (rows_at(0, i), mid)
            ov[at] = ov[at] - (gov[at] + rbl[at]) * inv
            at = p + (rows_at(K, i), mid)
            ov[at] = ov[at] - gov[at] * inv

        sweep(body)
        if not final:
            ups.append(send(ov.at[p + (top, mid)], new.at[p + (outer, mid)], over))

    def use_bottom(p):
        for copy in lows[p]:
            copy.wait_recv()

        def body(i):
            inv, at = scale[0:1, :], p + (rows_at(K, i),)
            ov[at + (first,)] = ov[at + (first,)] - (gov[at + (first,)] + from_left[at]) * inv
            if not final:
                rv[at] = rv[at] - (grv[at] + from_right[at]) * inv

        sweep(body)

    def use_top(p):
        for copy in tops[p]:
            copy.wait_recv()

        def body(i):
            inv, at = scale[0:1, :], p + (rows_at(0, i),)
            if final:
                mine = gov[at + (first,)] + rbl[at + (first,)]
            else:
                mine = tl[at]
                rv[at] = rv[at] - (tr[at] + from_right[at]) * inv
            ov[at + (first,)] = ov[at + (first,)] - (mine + from_left[at]) * inv

        sweep(body)
        n = len(outs)
        outs.append(pltpu.make_async_copy(ov.at[p], new.at[p + (whole, whole)], ls.at[4 + n]))
        if not final:
            ups.append(send(ov.at[p + (top, first)], new.at[p + (outer, first)], over))
            ups.append(send(rv.at[p + (top,)], new.at[p + (outer, outer)], over))
            outs.append(pltpu.make_async_copy(rv.at[p], new.at[p + (whole, outer)], ls.at[5 + n]))
        for copy in outs[n:]:
            copy.start()

    def settle(_):
        for copy in ups:
            copy.wait_recv()
        for copy in outs:
            copy.wait()

    reduce_run = reduce_steps()
    acts = {"d": down, "b": bottom, "m": middle, "L": ready, "t": send_top, "M": use_middle, "B": use_bottom, "T": use_top, "U": settle}
    done = {}
    for turn in ORDER[final]:
        if turn == "r":
            next(reduce_run, None)
        else:
            done[turn] = done.get(turn, -1) + 1
            acts[turn](PLANES[done[turn]])
    for _ in reduce_run:
        pass
    net.finish()


def run_exchange(final, es, beam, grads, ext):
    tile = 2 * K
    vmem = pl.BlockSpec(memory_space=pltpu.VMEM)
    anyw = pl.BlockSpec(memory_space=pl.ANY)
    shape = jax.ShapeDtypeStruct
    square, strip = pltpu.VMEM((2, 2, tile, tile), F32), pltpu.VMEM((2, 2, tile, K), F32)
    flat, small = pltpu.VMEM((2, 2, K, tile), F32), pltpu.VMEM((2, 2, K, K), F32)
    scratch = [square, strip, square, small, flat, strip, small] + ([] if final else [strip, strip, small])
    scratch += [
        pltpu.VMEM((8, K), F32),
        pltpu.VMEM((UNITS // 2, 8, HALF), F32),
        pltpu.VMEM((UNITS // 2, 8, HALF), F32),
        pltpu.VMEM((3, UNITS // 8, 8, HALF), F32),
        pltpu.VMEM((UNITS // 8, 8, HALF), F32),
        pltpu.VMEM((3, UNITS // 32, 8, HALF), F32),
        pltpu.VMEM((4, UNITS // 32, 8, HALF), F32),
        pltpu.VMEM((UNITS, 8, HALF), F32),
        pltpu.SemaphoreType.DMA((64,)),
        pltpu.SemaphoreType.DMA((64,)),
        pltpu.SemaphoreType.DMA((12,)),
    ]
    edge = tile if final else 3 * K
    return pl.pallas_call(
        functools.partial(exchange_kernel, final),
        out_shape=[shape(beam.shape, F32), shape((2, 2, edge, edge), F32)],
        in_specs=[vmem, vmem, anyw, anyw],
        out_specs=[vmem, anyw],
        scratch_shapes=scratch,
        compiler_params=pltpu.CompilerParams(
            collective_id=1 if final else 0, has_side_effects=True, vmem_limit_bytes=48 << 20
        ),
        name="close" if final else "exchange",
    )(es, beam, grads, ext)


def shards(object_field, probe, kernel_phase, measured, positions, batch):
    tile = object_field.shape[2]
    tables = constants()
    phase = even_odd(kernel_phase)
    kern = jnp.stack([jnp.cos(phase), jnp.sin(phase)])
    meas = even_odd(measured)
    corner = jnp.stack([lax.axis_index("tile") * tile, lax.axis_index("slab") * tile])
    local_at = positions - corner[None, :].astype(jnp.int32)
    beam = probe.reshape(2, K, 2, HALF).transpose(0, 2, 1, 3)
    ext = run_open(object_field)
    for batch_no in range(BATCHES):
        grads, es = run_batch(batch_no, local_at, batch, ext, beam, kern, meas, tables)
        flat, ext = run_exchange(
            batch_no + 1 == BATCHES, es.reshape(UNITS, 8, HALF), beam.reshape(UNITS * 2 // 3, 8, HALF), grads, ext
        )
        beam = flat.reshape(2, 2, K, HALF)
    return (ext, beam.transpose(0, 2, 1, 3).reshape(2, K, K))


def solution(mesh):
    in_specs = (
        P(None, None, "tile", "slab"),
        P(),
        P(),
        P(("tile", "slab"), None, None),
        P(("tile", "slab"), None),
        P(("tile", "slab")),
    )
    out_specs = (P(None, None, "tile", "slab"), P())
    return jax.shard_map(shards, mesh=mesh, in_specs=in_specs, out_specs=out_specs, check_vma=False)
```

```python
import functools
import math

import jax
import jax.numpy as jnp
import numpy as np
from jax import lax
from jax.experimental import pallas as pl
from jax.experimental.pallas import tpu as pltpu
from jax.sharding import PartitionSpec as P

BATCHES = 2
K = 256
HALF = 128
F32 = jnp.float32
BF16 = jnp.bfloat16


def bf16_pair(table):
    table = jnp.asarray(table, F32)
    high = table.astype(BF16)
    low = (table - high.astype(F32)).astype(BF16)
    return high, low


def constants():
    index = np.arange(HALF)
    angle = 2.0 * np.pi * (np.outer(index, index) % HALF) / HALF
    cos, sin = np.cos(angle) / 16.0, -np.sin(angle) / 16.0
    right = np.block([[cos, sin], [-sin, cos]])
    right_inv = np.block([[cos, -sin], [sin, cos]])
    rights, lefts = [], []
    for table in (right, right_inv):
        high, low = bf16_pair(table)
        rights.append(jnp.concatenate([high, low, high], axis=0))
        high, low = bf16_pair(table.T)
        lefts.append(jnp.concatenate([high, low, high], axis=1))
    twist = 2.0 * np.pi * index / K
    wr, wi = np.cos(twist).astype(np.float32), -np.sin(twist).astype(np.float32)
    lanes = jnp.asarray(np.stack([np.broadcast_to(wr, (8, HALF)), np.broadcast_to(wi, (8, HALF))]))
    rows = jnp.asarray(np.stack([np.broadcast_to(wr[:, None], (HALF, HALF)), np.broadcast_to(wi[:, None], (HALF, HALF))]))
    return (jnp.stack(rights), jnp.stack(lefts), lanes, rows)


def even_odd_table():
    order = np.concatenate([np.arange(0, K, 2), np.arange(1, K, 2)])
    pick = np.zeros((K, K), np.float32)
    pick[np.arange(K), order] = 1.0
    return jnp.asarray(np.stack([pick, pick.T]), BF16)


def three_parts(value):
    parts = []
    for _ in range(3):
        part = value.astype(BF16)
        parts.append(part)
        value = value - part.astype(F32)
    return parts


def even_odd(value, pick_ref):
    moved = sum(jnp.dot(pick_ref[0], part, preferred_element_type=F32) for part in three_parts(value))
    return sum(jnp.dot(part, pick_ref[1], preferred_element_type=F32) for part in three_parts(moved))


def batch_kernel(
    batch_no, at_ref, which_ref, ext, beam_ref, kern_ref, meas_hbm, mr_ref, ml_ref, wl_ref, wr_ref,
    g_out, es_ref,
    grad, window, meas_ref, patch, quantity, vr, vl, chosen, sems,
):
    count = jnp.int32(0)
    for f in range(which_ref.shape[0]):
        mine = which_ref[f] == batch_no

        @pl.when(mine)
        def _():
            chosen[count] = f

        count = count + mine.astype(jnp.int32)

    def corner_of(f):
        row, col = at_ref[f, 0], at_ref[f, 1]
        return pl.multiple_of((row // 8) * 8, 8), pl.multiple_of((col // HALF) * HALF, HALF)

    def fetches(n):
        f, slot = chosen[n], lax.rem(n, 2)
        row_base, col_base = corner_of(f)
        return (
            pltpu.make_async_copy(
                ext.at[:, :, pl.ds(row_base, K + 8), pl.ds(col_base, K + HALF)], window.at[slot], sems.at[slot]
            ),
            pltpu.make_async_copy(meas_hbm.at[f], meas_ref.at[slot], sems.at[2 + slot]),
        )

    def fetch(n):
        @pl.when(n < count)
        def _():
            for copy in fetches(n):
                copy.start()

    fetch(jnp.int32(0))

    def returns(layer):
        return [pltpu.make_async_copy(grad.at[c, layer], g_out.at[c, layer], sems.at[4 + 2 * c + layer]) for c in range(2)]

    def clear(i, carry):
        rows = pl.ds(pl.multiple_of(i * 64, 64), 64)
        for c in range(2):
            for layer in range(2):
                grad[c, layer, rows, :] = jnp.zeros((64, 3 * K), F32)
        return carry

    lax.fori_loop(0, 12, clear, 0)
    es_ref[...] = jnp.zeros_like(es_ref)

    lane = lax.broadcasted_iota(jnp.int32, (8, HALF), 1)
    sub = lax.broadcasted_iota(jnp.int32, (8, HALF), 0)
    lo, hi = slice(0, HALF), slice(HALF, K)

    def operand(blocks):
        highs = [[block.astype(BF16) for block in row] for row in blocks]
        lows = [
            [(block - high.astype(F32)).astype(BF16) for block, high in zip(row, parts)] for row, parts in zip(blocks, highs)
        ]
        return [jnp.concatenate([jnp.concatenate(row, axis=1) for row in rows], axis=0) for rows in (highs, lows)]

    def dot_right(inverse, cb, blocks):
        high, low = operand(blocks)
        vr[cb] = jnp.dot(jnp.concatenate([high, high, low], axis=1), mr_ref[inverse], preferred_element_type=F32)

    def dot_left(inverse, cb, blocks):
        high, low = operand(blocks)
        vl[cb] = jnp.dot(ml_ref[inverse], jnp.concatenate([high, high, low], axis=0), preferred_element_type=F32)

    def right_in(ar, ai, br, bi):
        wr, wi = wl_ref[0, 0:1, :], wl_ref[1, 0:1, :]
        dr, di = ar - br, ai - bi
        return [ar + br, ai + bi], [dr * wr - di * wi, dr * wi + di * wr]

    def right_out(i, n):
        wr, wi = wl_ref[0, 0:1, :], wl_ref[1, 0:1, :]
        rows = slice(i, i + n)
        er, ei, our, oi = vr[0, rows, lo], vr[0, rows, hi], vr[1, rows, lo], vr[1, rows, hi]
        tr, ti = our * wr + oi * wi, oi * wr - our * wi
        return er + tr, ei + ti, er - tr, ei - ti

    def left_in(cb):
        tops, lows = [], []
        for i in range(0, HALF, 32):
            wr, wi = wr_ref[0, i : i + 32, :], wr_ref[1, i : i + 32, :]
            top, low = slice(i, i + 32), slice(HALF + i, HALF + i + 32)
            ar, ai, br, bi = vr[cb, top, lo], vr[cb, top, hi], vr[cb, low, lo], vr[cb, low, hi]
            dr, di = ar - br, ai - bi
            tops.append([ar + br, dr * wr - di * wi])
            lows.append([ai + bi, dr * wi + di * wr])
        return tops + lows

    def left_out(cb):
        tops, lows = [], []
        for i in range(0, HALF, 32):
            wr, wi = wr_ref[0, i : i + 32, :], wr_ref[1, i : i + 32, :]
            top, low = slice(i, i + 32), slice(HALF + i, HALF + i + 32)
            er, ei, our, oi = vl[cb, top, lo], vl[cb, low, lo], vl[cb, top, hi], vl[cb, low, hi]
            tr, ti = our * wr + oi * wi, oi * wr - our * wi
            tops.append([er + tr, ei + ti])
            lows.append([er - tr, ei - ti])
        return tops + lows

    def at_frequency(change, cb):
        tops, lows = [], []
        for i in range(0, HALF, 32):
            pair = []
            for kb, cols in enumerate((lo, hi)):
                top, low = slice(i, i + 32), slice(HALF + i, HALF + i + 32)
                at = (slice(kb * HALF + i, kb * HALF + i + 32), slice(cb * HALF, cb * HALF + HALF))
                pair.append(change(vl[cb, top, cols], vl[cb, low, cols], at))
            tops.append([pair[0][0], pair[1][0]])
            lows.append([pair[0][1], pair[1][1]])
        return tops + lows

    def both_ways(change, evens, odds):
        dot_right(0, 0, evens)
        dot_right(0, 1, odds)
        for cb in range(2):
            dot_left(0, cb, left_in(cb))
        for cb in range(2):
            dot_left(1, cb, at_frequency(change, cb))
        for cb in range(2):
            dot_right(1, cb, left_out(cb))

    def propagate(re, im, at):
        kr, ki = kern_ref[0][at], kern_ref[1][at]
        return re * kr - im * ki, re * ki + im * kr

    def propagate_back(re, im, at):
        kr, ki = kern_ref[0][at], kern_ref[1][at]
        return re * kr + im * ki, im * kr - re * ki

    def frame(n, carry):
        if n is not None:
            f, slot = chosen[n], lax.rem(n, 2)
            fetch(n + 1)
            for copy in fetches(n):
                copy.wait()
            row, col = at_ref[f, 0], at_ref[f, 1]
            row_base, col_base = corner_of(f)
            down, off = row - row_base, col - col_base
            up, back = lax.rem(8 - down, 8), lax.rem(HALF - off, HALF)
            keep, keep_row = lane < HALF - off, sub < 8 - down
            inside, inside_row = lane >= off, sub >= down
            zero = jnp.zeros((8, HALF), F32)

            def target(i, j):
                return pl.ds(pl.multiple_of(row_base + i, 8), 8), pl.ds(pl.multiple_of(col_base + j * HALF, HALF), HALF)

            def cut(step, carry):
                i = step * 32
                for c in range(2):
                    for layer in range(2):
                        columns = []
                        for j in range(3):
                            turned = [
                                pltpu.roll(
                                    pltpu.roll(
                                        window[slot, c, layer, pl.ds(pl.multiple_of(i + 8 * k, 8), 8), HALF * j : HALF * (j + 1)],
                                        back, 1,
                                    ),
                                    up, 0,
                                )
                                for k in range(5)
                            ]
                            columns.append([jnp.where(keep_row, turned[k], turned[k + 1]) for k in range(4)])
                        for k in range(4):
                            at = pl.ds(pl.multiple_of(i + 8 * k, 8), 8)
                            patch[c, layer, at, lo] = jnp.where(keep, columns[0][k], columns[1][k])
                            patch[c, layer, at, hi] = jnp.where(keep, columns[1][k], columns[2][k])
                return carry

            lax.fori_loop(0, K // 32, cut, 0)

            def place(layer, i, half_r, half_i):
                for c, halves in enumerate((half_r, half_i)):
                    turned = [
                        [pltpu.roll(pltpu.roll(half[8 * k : 8 * k + 8], off, 1), down, 0) for k in range(4)] for half in halves
                    ]
                    left, right = [
                        [
                            jnp.where(inside_row, side[k] if k < 4 else zero, side[k - 1] if k else zero)
                            for k in range(5)
                        ]
                        for side in turned
                    ]
                    for k in range(5):
                        adds = (
                            jnp.where(inside, left[k], zero),
                            jnp.where(inside, right[k], left[k]),
                            jnp.where(inside, zero, right[k]),
                        )
                        for j, add in enumerate(adds):
                            at = (c, layer) + target(i + 8 * k, j)
                            grad[at] = grad[at] + add

            evens, odds = [], []
            for i in range(0, K, 32):
                rows = slice(i, i + 32)
                waves = []
                for n, cols in enumerate((lo, hi)):
                    br, bi = beam_ref[0, n, rows, :], beam_ref[1, n, rows, :]
                    pr, pi = patch[0, 0, rows, cols], patch[1, 0, rows, cols]
                    waves += [br * pr - bi * pi, br * pi + bi * pr]
                    es_ref[2, n, rows, :] = es_ref[2, n, rows, :] + (pr * pr + pi * pi)
                even, odd = right_in(*waves)
                evens.append(even)
                odds.append(odd)
            both_ways(propagate, evens, odds)
            evens, odds = [], []
            for i in range(0, K, 32):
                rows = slice(i, i + 32)
                qs = right_out(i, 32)
                waves = []
                for n, cols in enumerate((lo, hi)):
                    qr, qi = qs[2 * n], qs[2 * n + 1]
                    quantity[0, rows, cols] = qr
                    quantity[1, rows, cols] = qi
                    pr, pi = patch[0, 1, rows, cols], patch[1, 1, rows, cols]
                    waves += [pr * qr - pi * qi, pr * qi + pi * qr]
                even, odd = right_in(*waves)
                evens.append(even)
                odds.append(odd)
            def residual(re, im, at):
                power = re * re + im * im
                factor = 1.0 - meas_ref[slot, at[0], at[1]] * lax.rsqrt(jnp.maximum(power, 0.01))
                return re * factor, im * factor

            both_ways(residual, evens, odds)
            evens, odds = [], []
            for i in range(0, K, 32):
                rows = slice(i, i + 32)
                gs = right_out(i, 32)
                waves, dr, di = [], [], []
                for n, cols in enumerate((lo, hi)):
                    gr, gi = gs[2 * n], gs[2 * n + 1]
                    qr, qi = quantity[0, rows, cols], quantity[1, rows, cols]
                    pr, pi = patch[0, 1, rows, cols], patch[1, 1, rows, cols]
                    dr.append(qr * gr + qi * gi)
                    di.append(qr * gi - qi * gr)
                    waves += [pr * gr + pi * gi, pr * gi - pi * gr]
                even, odd = right_in(*waves)
                evens.append(even)
                odds.append(odd)
                place(1, i, dr, di)

            both_ways(propagate_back, evens, odds)
            evens, odds = [], []
            for i in range(0, K, 32):
                rows = slice(i, i + 32)
                gs = right_out(i, 32)
                dr, di = [], []
                for n, cols in enumerate((lo, hi)):
                    gr, gi = gs[2 * n], gs[2 * n + 1]
                    br, bi = beam_ref[0, n, rows, :], beam_ref[1, n, rows, :]
                    pr, pi = patch[0, 0, rows, cols], patch[1, 0, rows, cols]
                    dr.append(br * gr + bi * gi)
                    di.append(br * gi - bi * gr)
                    es_ref[0, n, rows, :] = es_ref[0, n, rows, :] + (pr * gr + pi * gi)
                    es_ref[1, n, rows, :] = es_ref[1, n, rows, :] + (pr * gi - pi * gr)
                place(0, i, dr, di)

        return carry

    lax.fori_loop(0, count, frame, 0)

    for copy in returns(0) + returns(1):
        copy.start()
    for copy in returns(0) + returns(1):
        copy.wait()


def run_batch(batch_no, local_at, batch, ext, beam, kern, meas, tables):
    smem = pl.BlockSpec(memory_space=pltpu.SMEM)
    vmem = pl.BlockSpec(memory_space=pltpu.VMEM)
    anyw = pl.BlockSpec(memory_space=pl.ANY)
    return pl.pallas_call(
        functools.partial(batch_kernel, batch_no),
        out_shape=[jax.ShapeDtypeStruct((2, 2, 3 * K, 3 * K), F32), jax.ShapeDtypeStruct((3, 2, K, HALF), F32)],
        in_specs=[smem, smem, anyw, vmem, vmem, anyw] + [vmem] * 4,
        out_specs=[anyw, vmem],
        scratch_shapes=[
            pltpu.VMEM((2, 2, 3 * K, 3 * K), F32),
            pltpu.VMEM((2, 2, 2, K + 8, K + HALF), F32),
            pltpu.VMEM((2, K, K), F32),
            pltpu.VMEM((2, 2, K, K), F32),
            pltpu.VMEM((2, K, K), F32),
            pltpu.VMEM((2, K, K), F32),
            pltpu.VMEM((2, K, K), F32),
            pltpu.SMEM((4,), jnp.int32),
            pltpu.SemaphoreType.DMA((8,)),
        ],
        compiler_params=pltpu.CompilerParams(vmem_limit_bytes=48 << 20),
        cost_estimate=pl.CostEstimate(flops=20_000_000_000, bytes_accessed=24 << 20, transcendentals=0),
        name="frames",
    )(local_at, batch, ext, beam, kern, meas, *tables)


MESH = pl.DeviceIdType.MESH
UNITS = 3 * K * K // (8 * HALF)


ORDER = {
    False: "rbrrdbrdbrdbLdtrmttrtmmmMrMMMBBBBTTTTU",
    True: "rsbrrdfrbdrdLfrtdtfmtmfrtmmMMMrMBBTTBBTTU",
}
PLANES = [(0, 0), (1, 0), (0, 1), (1, 1)]


class Net:
    def __init__(self, send_sems, recv_sems):
        self.t, self.y = t, y = lax.axis_index("tile"), lax.axis_index("slab")
        self.core, self.x, self.z = lax.rem(t, 2), lax.rem(t // 2, 4), t // 8
        self.partner = (t + 1 - 2 * self.core, y)
        self.under, self.over = (lax.rem(t + 1, 32), y), (lax.rem(t + 31, 32), y)
        self.rightward, self.leftward = (t, lax.rem(y + 1, 4)), (t, lax.rem(y + 3, 4))
        self.sems, self.sent = (send_sems, recv_sems), []

    def send(self, src, dst, device):
        n = len(self.sent)
        copy = pltpu.make_async_remote_copy(
            src_ref=src, dst_ref=dst, send_sem=self.sems[0].at[n], recv_sem=self.sems[1].at[n],
            device_id=device, device_id_type=MESH,
        )
        copy.start()
        self.sent.append(copy)
        return copy

    def meet(self, peers):
        barrier = pltpu.get_barrier_semaphore()
        for peer in peers:
            pl.semaphore_signal(barrier, inc=1, device_id=peer, device_id_type=MESH)
        pl.semaphore_wait(barrier, len(peers))

    def finish(self):
        for copy in self.sent:
            copy.wait_send()


LONG = 2


class Relay:
    def __init__(self, net, first, second, device, pieces):
        self.net, self.device, self.ways = net, device, (first, second)
        self.targets = [target for _, target in pieces]
        self.hops = [net.send(source, first.at[k], device) for k, (source, _) in enumerate(pieces)]
        self.at = 0

    def forward(self):
        stage, k = divmod(self.at, len(self.targets))
        self.at += 1
        self.hops[k].wait_recv()
        target = self.ways[1].at[k] if stage == 0 else self.targets[k]
        self.hops[k] = self.net.send(self.ways[stage].at[k], target, self.device)


def open_kernel(own, phase, meas, pick, ext, kern_out, meas_out, held, way1, way2, ss, rs, ls):
    net = Net(ss, rs)
    inward = [pltpu.make_async_copy(own.at[c, layer], held.at[c, layer], ls.at[2 * c + layer]) for c, layer in PLANES]
    for copy in inward:
        copy.start()
    net.meet([net.over, net.under, net.leftward, net.rightward])
    top, low, first = pl.ds(0, K), pl.ds(K, K), pl.ds(0, K)
    outer = pl.ds(2 * K, K)
    relay = Relay(net, way1, way2, net.rightward, [(own.at[p + (low, first)], ext.at[p + (low, outer)]) for p in PLANES[:LONG]])
    tops = [net.send(own.at[p + (top, first)], ext.at[p + (top, outer)], net.leftward) for p in PLANES]
    belows = [net.send(own.at[p + (top,)], ext.at[p + (outer, pl.ds(0, 2 * K))], net.over) for p in PLANES]
    lows = [net.send(own.at[p + (low, first)], ext.at[p + (low, outer)], net.leftward) for p in PLANES[LONG:]]
    for copy in inward:
        copy.wait()
    outward = [
        pltpu.make_async_copy(held.at[p], ext.at[p + (pl.ds(0, 2 * K), pl.ds(0, 2 * K))], ls.at[2 * p[0] + p[1]]) for p in PLANES
    ]
    for copy in outward:
        copy.start()
    corners = []

    def corner(n):
        tops[n].wait_recv()
        p = PLANES[n]
        corners.append(net.send(ext.at[p + (top, outer)], ext.at[p + (outer, outer)], net.over))

    def reorder(f):
        meas_out[f] = even_odd(meas[f], pick)

    relay.forward()
    corner(0)
    turned = even_odd(phase[...], pick)
    kern_out[0] = jnp.cos(turned)
    kern_out[1] = jnp.sin(turned)
    relay.forward()
    corner(1)
    reorder(0)
    relay.forward()
    corner(2)
    reorder(1)
    reorder(2)
    relay.forward()
    corner(3)
    reorder(3)
    for copy in belows + lows + corners + relay.hops:
        copy.wait_recv()
    for copy in outward:
        copy.wait()
    net.finish()


def run_open(own, phase, meas):
    vmem = pl.BlockSpec(memory_space=pltpu.VMEM)
    anyw = pl.BlockSpec(memory_space=pl.ANY)
    shape = jax.ShapeDtypeStruct
    return pl.pallas_call(
        open_kernel,
        out_shape=[shape((2, 2, 3 * K, 3 * K), F32), shape((2, K, K), F32), shape(meas.shape, F32)],
        in_specs=[anyw, vmem, vmem, vmem],
        out_specs=[anyw, vmem, vmem],
        scratch_shapes=[
            pltpu.VMEM((2, 2, 2 * K, 2 * K), F32),
            pltpu.VMEM((LONG, K, K), F32),
            pltpu.VMEM((LONG, K, K), F32),
            pltpu.SemaphoreType.DMA((24,)),
            pltpu.SemaphoreType.DMA((24,)),
            pltpu.SemaphoreType.DMA((4,)),
        ],
        compiler_params=pltpu.CompilerParams(collective_id=2, has_side_effects=True, vmem_limit_bytes=48 << 20),
        name="open",
    )(own, phase, meas, even_odd_table())


def exchange_kernel(final, *refs):
    es, beam, g, ext, beam_new, new = refs[:6]
    gov, grv, ov, rx, rbl, from_left, tr = refs[6:13]
    rest = refs[13:]
    if final:
        way1, way2 = rest[:2]
        rest = rest[2:]
    else:
        rv, from_right, tl = rest[:3]
        rest = rest[3:]
    scale, rc, acc, rz, acc2, rxs, rys, total, ss, rs, ls = rest
    net = Net(ss, rs)
    core, x, y, z, partner, send = net.core, net.x, net.y, net.z, net.partner, net.send
    under, over, rightward, leftward = net.under, net.over, net.rightward, net.leftward

    def zpeer(d):
        zp = lax.rem(z + d, 4)
        return zp, ((zp * 4 + x) * 2 + core, y)

    def xpeer(d):
        xp = lax.rem(x + d, 4)
        return xp, ((z * 4 + xp) * 2 + core, y)

    def ypeer(d):
        yp = lax.rem(y + d, 4)
        return yp, (net.t, yp)

    whole, outer = pl.ds(0, 2 * K), pl.ds(2 * K, K)
    square, strip = (slice(None), slice(None), whole, whole), (slice(None), slice(None), whole, outer)
    local = [
        pltpu.make_async_copy(g.at[square], gov, ls.at[0]),
        pltpu.make_async_copy(g.at[strip], grv, ls.at[1]),
        pltpu.make_async_copy(ext.at[square], ov, ls.at[2]),
    ]
    if not final:
        local.append(pltpu.make_async_copy(ext.at[strip], rv, ls.at[3]))
    for copy in local:
        copy.start()
    net.meet([partner, under, over] + [p(d)[1] for p in (zpeer, xpeer, ypeer) for d in (1, 2, 3)])

    def reduce_steps():
        half, quarter, part = UNITS // 2, UNITS // 8, UNITS // 32
        copy = send(es.at[pl.ds((1 - core) * half, half)], rc, partner)
        yield
        copy.wait_recv()
        acc[...] = es[pl.ds(core * half, half)] + rc[...]
        copies = []
        for d in (1, 2, 3):
            zp, peer = zpeer(d)
            copies.append(send(acc.at[pl.ds(zp * quarter, quarter)], rz.at[d - 1], peer))
        yield
        for copy in copies:
            copy.wait_recv()
        acc2[...] = acc[pl.ds(z * quarter, quarter)] + (rz[0] + rz[1] + rz[2])
        copies = []
        for d in (1, 2, 3):
            xp, peer = xpeer(d)
            copies.append(send(acc2.at[pl.ds(xp * part, part)], rxs.at[d - 1], peer))
        yield
        for copy in copies:
            copy.wait_recv()
        rys[y] = acc2[pl.ds(x * part, part)] + (rxs[0] + rxs[1] + rxs[2])
        copies = [send(rys.at[y], rys.at[y], ypeer(d)[1]) for d in (1, 2, 3)]
        yield
        for copy in copies:
            copy.wait_recv()
        base = core * half + z * quarter + x * part
        total[pl.ds(base, part)] = (rys[0] + rys[1]) + (rys[2] + rys[3])
        for start, size, targets in (
            (base, part, [xpeer(d)[1] for d in (1, 2, 3)]),
            (core * half + z * quarter, quarter, [zpeer(d)[1] for d in (1, 2, 3)]),
            (core * half, half, [partner]),
        ):
            piece = total.at[pl.ds(start, size)]
            copies = [send(piece, piece, peer) for peer in targets]
            yield
            for copy in copies:
                copy.wait_recv()
        units = UNITS // 3
        for c in range(2):
            at = pl.ds(c * units, units)
            beam_new[at] = beam[at] - total[at] / (total[pl.ds(2 * units, units)] + 1.0)

    top, low = pl.ds(0, K), pl.ds(K, K)
    first, mid = pl.ds(0, K), pl.ds(K, K)

    def sweep(body):
        def step(i, carry):
            body(i * 32)
            return carry

        lax.fori_loop(0, K // 32, step, 0)

    def rows_at(base, i):
        return pl.ds(pl.multiple_of(base + i, 32), 32)

    corners, mids, lows, tops, ups, outs = {}, {}, {}, {}, [], []

    def down(p):
        corners[p] = (
            send(g.at[p + (outer, outer)], rx.at[p], under),
            send(g.at[p + (outer, first)], rbl.at[p + (slice(None), first)], under),
        )

    relays = []

    def start_relay(_):
        pieces = [(g.at[p + (low, outer)], from_left.at[p + (low,)]) for p in PLANES[:LONG]]
        relays.append(Relay(net, way1, way2, leftward, pieces))

    def forward(_):
        relays[0].forward()

    def bottom(p):
        lows[p] = [send(g.at[p + (low, outer)], from_left.at[p + (low,)], rightward)]
        if not final:
            lows[p].append(send(g.at[p + (low, first)], from_right.at[p + (low,)], leftward))

    def middle(p):
        mids[p] = send(g.at[p + (outer, mid)], rbl.at[p + (slice(None), mid)], under)

    def ready(_):
        for copy in local:
            copy.wait()
        units = UNITS // 3
        power = jnp.max(beam[pl.ds(0, units)] ** 2 + beam[pl.ds(units, units)] ** 2, axis=0)
        peak = jnp.max(jnp.max(power, axis=0, keepdims=True), axis=1, keepdims=True)
        scale[...] = jnp.broadcast_to(1.0 / peak, (8, K))

    def send_top(p):
        for copy in corners[p]:
            copy.wait_recv()

        def body(i):
            at = p + (rows_at(0, i),)
            tr[at] = grv[at] + rx[at]
            if not final:
                tl[at] = gov[at + (first,)] + rbl[at + (first,)]

        sweep(body)
        tops[p] = [send(tr.at[p], from_left.at[p + (top,)], rightward)]
        if not final:
            tops[p].append(send(tl.at[p], from_right.at[p + (top,)], leftward))

    def use_middle(p):
        mids[p].wait_recv()

        def body(i):
            inv = scale[0:1, :]
            at = p + (rows_at(0, i), mid)
            ov[at] = ov[at] - (gov[at] + rbl[at]) * inv
            at = p + (rows_at(K, i), mid)
            ov[at] = ov[at] - gov[at] * inv

        sweep(body)
        if not final:
            ups.append(send(ov.at[p + (top, mid)], new.at[p + (outer, mid)], over))

    def use_bottom(p):
        for copy in lows[p] if p in lows else [relays[0].hops[PLANES.index(p)]]:
            copy.wait_recv()

        def body(i):
            inv, at = scale[0:1, :], p + (rows_at(K, i),)
            ov[at + (first,)] = ov[at + (first,)] - (gov[at + (first,)] + from_left[at]) * inv
            if not final:
                rv[at] = rv[at] - (grv[at] + from_right[at]) * inv

        sweep(body)

    def use_top(p):
        for copy in tops[p]:
            copy.wait_recv()

        def body(i):
            inv, at = scale[0:1, :], p + (rows_at(0, i),)
            if final:
                mine = gov[at + (first,)] + rbl[at + (first,)]
            else:
                mine = tl[at]
                rv[at] = rv[at] - (tr[at] + from_right[at]) * inv
            ov[at + (first,)] = ov[at + (first,)] - (mine + from_left[at]) * inv

        sweep(body)
        n = len(outs)
        outs.append(pltpu.make_async_copy(ov.at[p], new.at[p + (whole, whole)], ls.at[4 + n]))
        if not final:
            ups.append(send(ov.at[p + (top, first)], new.at[p + (outer, first)], over))
            ups.append(send(rv.at[p + (top,)], new.at[p + (outer, outer)], over))
            outs.append(pltpu.make_async_copy(rv.at[p], new.at[p + (whole, outer)], ls.at[5 + n]))
        for copy in outs[n:]:
            copy.start()

    def settle(_):
        for copy in ups:
            copy.wait_recv()
        for copy in outs:
            copy.wait()

    reduce_run = reduce_steps()
    acts = {"d": down, "b": bottom, "m": middle, "L": ready, "t": send_top, "M": use_middle, "B": use_bottom, "T": use_top, "U": settle}
    if final:
        acts.update({"s": start_relay, "f": forward})
    done = {"b": LONG - 1, "B": LONG - 1, "T": LONG - 1} if final else {}
    for turn in ORDER[final]:
        if turn == "r":
            next(reduce_run, None)
        else:
            done[turn] = done.get(turn, -1) + 1
            acts[turn](PLANES[done[turn] % 4])
    for _ in reduce_run:
        pass
    net.finish()


def run_exchange(final, es, beam, grads, ext):
    tile = 2 * K
    vmem = pl.BlockSpec(memory_space=pltpu.VMEM)
    anyw = pl.BlockSpec(memory_space=pl.ANY)
    shape = jax.ShapeDtypeStruct
    square, strip = pltpu.VMEM((2, 2, tile, tile), F32), pltpu.VMEM((2, 2, tile, K), F32)
    flat, small = pltpu.VMEM((2, 2, K, tile), F32), pltpu.VMEM((2, 2, K, K), F32)
    scratch = [square, strip, square, small, flat, strip, small] + ([pltpu.VMEM((LONG, K, K), F32)] * 2 if final else [strip, strip, small])
    scratch += [
        pltpu.VMEM((8, K), F32),
        pltpu.VMEM((UNITS // 2, 8, HALF), F32),
        pltpu.VMEM((UNITS // 2, 8, HALF), F32),
        pltpu.VMEM((3, UNITS // 8, 8, HALF), F32),
        pltpu.VMEM((UNITS // 8, 8, HALF), F32),
        pltpu.VMEM((3, UNITS // 32, 8, HALF), F32),
        pltpu.VMEM((4, UNITS // 32, 8, HALF), F32),
        pltpu.VMEM((UNITS, 8, HALF), F32),
        pltpu.SemaphoreType.DMA((64,)),
        pltpu.SemaphoreType.DMA((64,)),
        pltpu.SemaphoreType.DMA((12,)),
    ]
    edge = tile if final else 3 * K
    return pl.pallas_call(
        functools.partial(exchange_kernel, final),
        out_shape=[shape(beam.shape, F32), shape((2, 2, edge, edge), F32)],
        in_specs=[vmem, vmem, anyw, anyw],
        out_specs=[vmem, anyw],
        scratch_shapes=scratch,
        compiler_params=pltpu.CompilerParams(
            collective_id=1 if final else 0, has_side_effects=True, vmem_limit_bytes=48 << 20
        ),
        name="close" if final else "exchange",
    )(es, beam, grads, ext)


def shards(object_field, probe, kernel_phase, measured, positions, batch):
    tile = object_field.shape[2]
    tables = constants()
    corner = jnp.stack([lax.axis_index("tile") * tile, lax.axis_index("slab") * tile])
    local_at = positions - corner[None, :].astype(jnp.int32)
    beam = probe.reshape(2, K, 2, HALF).transpose(0, 2, 1, 3)
    ext, kern, meas = run_open(object_field, kernel_phase, measured)
    for batch_no in range(BATCHES):
        grads, es = run_batch(batch_no, local_at, batch, ext, beam, kern, meas, tables)
        flat, ext = run_exchange(
            batch_no + 1 == BATCHES, es.reshape(UNITS, 8, HALF), beam.reshape(UNITS * 2 // 3, 8, HALF), grads, ext
        )
        beam = flat.reshape(2, 2, K, HALF)
    return (ext, beam.transpose(0, 2, 1, 3).reshape(2, K, K))


def solution(mesh):
    in_specs = (
        P(None, None, "tile", "slab"),
        P(),
        P(),
        P(("tile", "slab"), None, None),
        P(("tile", "slab"), None),
        P(("tile", "slab")),
    )
    out_specs = (P(None, None, "tile", "slab"), P())
    return jax.shard_map(shards, mesh=mesh, in_specs=in_specs, out_specs=out_specs, check_vma=False)
```

```python
import functools
import math

import jax
import jax.numpy as jnp
import numpy as np
from jax import lax
from jax.experimental import pallas as pl
from jax.experimental.pallas import tpu as pltpu
from jax.sharding import PartitionSpec as P

BATCHES = 2
K = 256
HALF = 128
F32 = jnp.float32
BF16 = jnp.bfloat16


def bf16_pair(table):
    table = jnp.asarray(table, F32)
    high = table.astype(BF16)
    low = (table - high.astype(F32)).astype(BF16)
    return high, low


def constants():
    index = np.arange(HALF)
    angle = 2.0 * np.pi * (np.outer(index, index) % HALF) / HALF
    cos, sin = np.cos(angle) / 16.0, -np.sin(angle) / 16.0
    right = np.block([[cos, sin], [-sin, cos]])
    right_inv = np.block([[cos, -sin], [sin, cos]])
    rights, lefts = [], []
    for table in (right, right_inv):
        high, low = bf16_pair(table)
        rights.append(jnp.concatenate([high, low, high], axis=0))
        high, low = bf16_pair(table.T)
        lefts.append(jnp.concatenate([high, low, high], axis=1))
    twist = 2.0 * np.pi * index / K
    wr, wi = np.cos(twist).astype(np.float32), -np.sin(twist).astype(np.float32)
    lanes = jnp.asarray(np.stack([np.broadcast_to(wr, (8, HALF)), np.broadcast_to(wi, (8, HALF))]))
    rows = jnp.asarray(np.stack([np.broadcast_to(wr[:, None], (HALF, HALF)), np.broadcast_to(wi[:, None], (HALF, HALF))]))
    return (jnp.stack(rights), jnp.stack(lefts), lanes, rows)


def fill_even_odd(pick):
    for n in range(2):
        new = lax.broadcasted_iota(jnp.int32, (K, K), n)
        old = lax.broadcasted_iota(jnp.int32, (K, K), 1 - n)
        hit = old == jnp.where(new < HALF, 2 * new, 2 * new - (K - 1))
        pick[n] = jnp.where(hit, 1.0, 0.0).astype(BF16)


def three_parts(value):
    parts = []
    for _ in range(3):
        part = value.astype(BF16)
        parts.append(part)
        value = value - part.astype(F32)
    return parts


def even_odd(value, pick_ref):
    moved = sum(jnp.dot(pick_ref[0], part, preferred_element_type=F32) for part in three_parts(value))
    return sum(jnp.dot(part, pick_ref[1], preferred_element_type=F32) for part in three_parts(moved))


def batch_kernel(
    batch_no, at_ref, which_ref, ext, beam_ref, kern_ref, meas_hbm, mr_ref, ml_ref, wl_ref, wr_ref,
    g_out, es_ref,
    grad, window, meas_ref, patch, quantity, vr, vl, chosen, sems,
):
    row_start, col_start = lax.axis_index("tile") * (2 * K), lax.axis_index("slab") * (2 * K)
    count = jnp.int32(0)
    for f in range(which_ref.shape[0]):
        mine = which_ref[f] == batch_no

        @pl.when(mine)
        def _():
            chosen[count] = f

        count = count + mine.astype(jnp.int32)

    def corner_of(f):
        row, col = at_ref[0, f] - row_start, at_ref[1, f] - col_start
        return pl.multiple_of((row // 8) * 8, 8), pl.multiple_of((col // HALF) * HALF, HALF)

    def fetches(n):
        f, slot = chosen[n], lax.rem(n, 2)
        row_base, col_base = corner_of(f)
        return (
            pltpu.make_async_copy(
                ext.at[:, :, pl.ds(row_base, K + 8), pl.ds(col_base, K + HALF)], window.at[slot], sems.at[slot]
            ),
            pltpu.make_async_copy(meas_hbm.at[f], meas_ref.at[slot], sems.at[2 + slot]),
        )

    def fetch(n):
        @pl.when(n < count)
        def _():
            for copy in fetches(n):
                copy.start()

    fetch(jnp.int32(0))
    def returns(layer):
        return [pltpu.make_async_copy(grad.at[c, layer], g_out.at[c, layer], sems.at[4 + 2 * c + layer]) for c in range(2)]

    def clear(i, carry):
        rows = pl.ds(pl.multiple_of(i * 64, 64), 64)
        for c in range(2):
            for layer in range(2):
                grad[c, layer, rows, :] = jnp.zeros((64, 3 * K), F32)
        return carry

    lax.fori_loop(0, 12, clear, 0)
    es_ref[...] = jnp.zeros_like(es_ref)
    lane = lax.broadcasted_iota(jnp.int32, (8, HALF), 1)
    sub = lax.broadcasted_iota(jnp.int32, (8, HALF), 0)
    lo, hi = slice(0, HALF), slice(HALF, K)

    def operand(blocks):
        highs = [[block.astype(BF16) for block in row] for row in blocks]
        lows = [
            [(block - high.astype(F32)).astype(BF16) for block, high in zip(row, parts)] for row, parts in zip(blocks, highs)
        ]
        return [jnp.concatenate([jnp.concatenate(row, axis=1) for row in rows], axis=0) for rows in (highs, lows)]

    def dot_right(inverse, cb, blocks):
        high, low = operand(blocks)
        vr[cb] = jnp.dot(jnp.concatenate([high, high, low], axis=1), mr_ref[inverse], preferred_element_type=F32)

    def dot_left(inverse, cb, blocks):
        high, low = operand(blocks)
        vl[cb] = jnp.dot(ml_ref[inverse], jnp.concatenate([high, high, low], axis=0), preferred_element_type=F32)

    def right_in(ar, ai, br, bi):
        wr, wi = wl_ref[0, 0:1, :], wl_ref[1, 0:1, :]
        dr, di = ar - br, ai - bi
        return [ar + br, ai + bi], [dr * wr - di * wi, dr * wi + di * wr]

    def right_out(i, n):
        wr, wi = wl_ref[0, 0:1, :], wl_ref[1, 0:1, :]
        rows = slice(i, i + n)
        er, ei, our, oi = vr[0, rows, lo], vr[0, rows, hi], vr[1, rows, lo], vr[1, rows, hi]
        tr, ti = our * wr + oi * wi, oi * wr - our * wi
        return er + tr, ei + ti, er - tr, ei - ti

    def left_in(cb):
        tops, lows = [], []
        for i in range(0, HALF, 32):
            wr, wi = wr_ref[0, i : i + 32, :], wr_ref[1, i : i + 32, :]
            top, low = slice(i, i + 32), slice(HALF + i, HALF + i + 32)
            ar, ai, br, bi = vr[cb, top, lo], vr[cb, top, hi], vr[cb, low, lo], vr[cb, low, hi]
            dr, di = ar - br, ai - bi
            tops.append([ar + br, dr * wr - di * wi])
            lows.append([ai + bi, dr * wi + di * wr])
        return tops + lows

    def left_out(cb):
        tops, lows = [], []
        for i in range(0, HALF, 32):
            wr, wi = wr_ref[0, i : i + 32, :], wr_ref[1, i : i + 32, :]
            top, low = slice(i, i + 32), slice(HALF + i, HALF + i + 32)
            er, ei, our, oi = vl[cb, top, lo], vl[cb, low, lo], vl[cb, top, hi], vl[cb, low, hi]
            tr, ti = our * wr + oi * wi, oi * wr - our * wi
            tops.append([er + tr, ei + ti])
            lows.append([er - tr, ei - ti])
        return tops + lows

    def at_frequency(change, cb):
        tops, lows = [], []
        for i in range(0, HALF, 32):
            pair = []
            for kb, cols in enumerate((lo, hi)):
                top, low = slice(i, i + 32), slice(HALF + i, HALF + i + 32)
                at = (slice(kb * HALF + i, kb * HALF + i + 32), slice(cb * HALF, cb * HALF + HALF))
                pair.append(change(vl[cb, top, cols], vl[cb, low, cols], at))
            tops.append([pair[0][0], pair[1][0]])
            lows.append([pair[0][1], pair[1][1]])
        return tops + lows

    def both_ways(change, evens, odds):
        dot_right(0, 0, evens)
        dot_right(0, 1, odds)
        for cb in range(2):
            dot_left(0, cb, left_in(cb))
        for cb in range(2):
            dot_left(1, cb, at_frequency(change, cb))
        for cb in range(2):
            dot_right(1, cb, left_out(cb))

    def propagate(re, im, at):
        kr, ki = kern_ref[0][at], kern_ref[1][at]
        return re * kr - im * ki, re * ki + im * kr

    def propagate_back(re, im, at):
        kr, ki = kern_ref[0][at], kern_ref[1][at]
        return re * kr + im * ki, im * kr - re * ki

    def frame(n, carry):
        if n is not None:
            f, slot = chosen[n], lax.rem(n, 2)
            fetch(n + 1)
            for copy in fetches(n):
                copy.wait()
            row, col = at_ref[0, f] - row_start, at_ref[1, f] - col_start
            row_base, col_base = corner_of(f)
            down, off = row - row_base, col - col_base
            up, back = lax.rem(8 - down, 8), lax.rem(HALF - off, HALF)
            keep, keep_row = lane < HALF - off, sub < 8 - down
            inside, inside_row = lane >= off, sub >= down
            zero = jnp.zeros((8, HALF), F32)

            def target(i, j):
                return pl.ds(pl.multiple_of(row_base + i, 8), 8), pl.ds(pl.multiple_of(col_base + j * HALF, HALF), HALF)

            def cut(step, carry):
                i = step * 32
                for c in range(2):
                    for layer in range(2):
                        columns = []
                        for j in range(3):
                            turned = [
                                pltpu.roll(
                                    pltpu.roll(
                                        window[slot, c, layer, pl.ds(pl.multiple_of(i + 8 * k, 8), 8), HALF * j : HALF * (j + 1)],
                                        back, 1,
                                    ),
                                    up, 0,
                                )
                                for k in range(5)
                            ]
                            columns.append([jnp.where(keep_row, turned[k], turned[k + 1]) for k in range(4)])
                        for k in range(4):
                            at = pl.ds(pl.multiple_of(i + 8 * k, 8), 8)
                            patch[c, layer, at, lo] = jnp.where(keep, columns[0][k], columns[1][k])
                            patch[c, layer, at, hi] = jnp.where(keep, columns[1][k], columns[2][k])
                return carry

            lax.fori_loop(0, K // 32, cut, 0)

            def place(layer, i, half_r, half_i):
                for c, halves in enumerate((half_r, half_i)):
                    turned = [
                        [pltpu.roll(pltpu.roll(half[8 * k : 8 * k + 8], off, 1), down, 0) for k in range(4)] for half in halves
                    ]
                    left, right = [
                        [
                            jnp.where(inside_row, side[k] if k < 4 else zero, side[k - 1] if k else zero)
                            for k in range(5)
                        ]
                        for side in turned
                    ]
                    for k in range(5):
                        adds = (
                            jnp.where(inside, left[k], zero),
                            jnp.where(inside, right[k], left[k]),
                            jnp.where(inside, zero, right[k]),
                        )
                        for j, add in enumerate(adds):
                            at = (c, layer) + target(i + 8 * k, j)
                            grad[at] = grad[at] + add

            evens, odds = [], []
            for i in range(0, K, 32):
                rows = slice(i, i + 32)
                waves = []
                for n, cols in enumerate((lo, hi)):
                    br, bi = beam_ref[0, n, rows, :], beam_ref[1, n, rows, :]
                    pr, pi = patch[0, 0, rows, cols], patch[1, 0, rows, cols]
                    waves += [br * pr - bi * pi, br * pi + bi * pr]
                    es_ref[2, n, rows, :] = es_ref[2, n, rows, :] + (pr * pr + pi * pi)
                even, odd = right_in(*waves)
                evens.append(even)
                odds.append(odd)
            both_ways(propagate, evens, odds)
            evens, odds = [], []
            for i in range(0, K, 32):
                rows = slice(i, i + 32)
                qs = right_out(i, 32)
                waves = []
                for n, cols in enumerate((lo, hi)):
                    qr, qi = qs[2 * n], qs[2 * n + 1]
                    quantity[0, rows, cols] = qr
                    quantity[1, rows, cols] = qi
                    pr, pi = patch[0, 1, rows, cols], patch[1, 1, rows, cols]
                    waves += [pr * qr - pi * qi, pr * qi + pi * qr]
                even, odd = right_in(*waves)
                evens.append(even)
                odds.append(odd)
            def residual(re, im, at):
                power = re * re + im * im
                factor = 1.0 - meas_ref[slot, at[0], at[1]] * lax.rsqrt(jnp.maximum(power, 0.01))
                return re * factor, im * factor

            both_ways(residual, evens, odds)
            evens, odds = [], []
            for i in range(0, K, 32):
                rows = slice(i, i + 32)
                gs = right_out(i, 32)
                waves, dr, di = [], [], []
                for n, cols in enumerate((lo, hi)):
                    gr, gi = gs[2 * n], gs[2 * n + 1]
                    qr, qi = quantity[0, rows, cols], quantity[1, rows, cols]
                    pr, pi = patch[0, 1, rows, cols], patch[1, 1, rows, cols]
                    dr.append(qr * gr + qi * gi)
                    di.append(qr * gi - qi * gr)
                    waves += [pr * gr + pi * gi, pr * gi - pi * gr]
                even, odd = right_in(*waves)
                evens.append(even)
                odds.append(odd)
                place(1, i, dr, di)

            both_ways(propagate_back, evens, odds)
            evens, odds = [], []
            for i in range(0, K, 32):
                rows = slice(i, i + 32)
                gs = right_out(i, 32)
                dr, di = [], []
                for n, cols in enumerate((lo, hi)):
                    gr, gi = gs[2 * n], gs[2 * n + 1]
                    br, bi = beam_ref[0, n, rows, :], beam_ref[1, n, rows, :]
                    pr, pi = patch[0, 0, rows, cols], patch[1, 0, rows, cols]
                    dr.append(br * gr + bi * gi)
                    di.append(br * gi - bi * gr)
                    es_ref[0, n, rows, :] = es_ref[0, n, rows, :] + (pr * gr + pi * gi)
                    es_ref[1, n, rows, :] = es_ref[1, n, rows, :] + (pr * gi - pi * gr)
                place(0, i, dr, di)

        return carry

    lax.fori_loop(0, count, frame, 0)

    for copy in returns(0) + returns(1):
        copy.start()
    for copy in returns(0) + returns(1):
        copy.wait()


def run_batch(batch_no, places, batch, ext, beam, kern, meas, tables):
    smem = pl.BlockSpec(memory_space=pltpu.SMEM)
    vmem = pl.BlockSpec(memory_space=pltpu.VMEM)
    anyw = pl.BlockSpec(memory_space=pl.ANY)
    return pl.pallas_call(
        functools.partial(batch_kernel, batch_no),
        out_shape=[jax.ShapeDtypeStruct((2, 2, 3 * K, 3 * K), F32), jax.ShapeDtypeStruct((3, 2, K, HALF), F32)],
        in_specs=[smem, smem, anyw, vmem, vmem, anyw] + [vmem] * 4,
        out_specs=[anyw, vmem],
        scratch_shapes=[
            pltpu.VMEM((2, 2, 3 * K, 3 * K), F32),
            pltpu.VMEM((2, 2, 2, K + 8, K + HALF), F32),
            pltpu.VMEM((2, K, K), F32),
            pltpu.VMEM((2, 2, K, K), F32),
            pltpu.VMEM((2, K, K), F32),
            pltpu.VMEM((2, K, K), F32),
            pltpu.VMEM((2, K, K), F32),
            pltpu.SMEM((4,), jnp.int32),
            pltpu.SemaphoreType.DMA((8,)),
        ],
        compiler_params=pltpu.CompilerParams(vmem_limit_bytes=48 << 20),
        cost_estimate=pl.CostEstimate(flops=20_000_000_000, bytes_accessed=24 << 20, transcendentals=0),
        name="frames",
    )(places, batch, ext, beam, kern, meas, *tables)


MESH = pl.DeviceIdType.MESH
UNITS = 3 * K * K // (8 * HALF)


ORDER = {
    False: "rbrrdbrdbrdbLdtrmttrtmmmMrMMMBBBBTTTTU",
    True: "rsbrrdfrbdrdLfrtdtfmtmfrtmmMMMrMBBTTBBTTU",
}
PLANES = [(0, 0), (1, 0), (0, 1), (1, 1)]


class Net:
    def __init__(self, send_sems, recv_sems):
        self.t, self.y = t, y = lax.axis_index("tile"), lax.axis_index("slab")
        self.core, self.x, self.z = lax.rem(t, 2), lax.rem(t // 2, 4), t // 8
        self.partner = (t + 1 - 2 * self.core, y)
        self.under, self.over = (lax.rem(t + 1, 32), y), (lax.rem(t + 31, 32), y)
        self.rightward, self.leftward = (t, lax.rem(y + 1, 4)), (t, lax.rem(y + 3, 4))
        self.sems, self.sent = (send_sems, recv_sems), []

    def send(self, src, dst, device):
        n = len(self.sent)
        copy = pltpu.make_async_remote_copy(
            src_ref=src, dst_ref=dst, send_sem=self.sems[0].at[n], recv_sem=self.sems[1].at[n],
            device_id=device, device_id_type=MESH,
        )
        copy.start()
        self.sent.append(copy)
        return copy

    def meet(self, peers):
        barrier = pltpu.get_barrier_semaphore()
        for peer in peers:
            pl.semaphore_signal(barrier, inc=1, device_id=peer, device_id_type=MESH)
        pl.semaphore_wait(barrier, len(peers))

    def finish(self):
        for copy in self.sent:
            copy.wait_send()


LONG = 2


class Relay:
    def __init__(self, net, first, second, device, pieces):
        self.net, self.device, self.ways = net, device, (first, second)
        self.targets = [target for _, target in pieces]
        self.hops = [net.send(source, first.at[k], device) for k, (source, _) in enumerate(pieces)]
        self.at = 0

    def forward(self):
        stage, k = divmod(self.at, len(self.targets))
        self.at += 1
        self.hops[k].wait_recv()
        target = self.ways[1].at[k] if stage == 0 else self.targets[k]
        self.hops[k] = self.net.send(self.ways[stage].at[k], target, self.device)


def open_kernel(
    own, phase_hbm, meas_hbm, probe_hbm, ext, kern_out, meas_out, beam_out,
    held, way1, way2, phase, meas, pick, probe, ss, rs, ls,
):
    net = Net(ss, rs)
    loads = [
        pltpu.make_async_copy(source, target, ls.at[4 + n])
        for n, (source, target) in enumerate(((phase_hbm, phase), (meas_hbm, meas), (probe_hbm, probe)))
    ]
    for copy in loads:
        copy.start()
    inward = [pltpu.make_async_copy(own.at[c, layer], held.at[c, layer], ls.at[2 * c + layer]) for c, layer in PLANES]
    for copy in inward:
        copy.start()
    net.meet([net.over, net.under, net.leftward, net.rightward])
    top, low, first = pl.ds(0, K), pl.ds(K, K), pl.ds(0, K)
    outer = pl.ds(2 * K, K)
    relay = Relay(net, way1, way2, net.rightward, [(own.at[p + (low, first)], ext.at[p + (low, outer)]) for p in PLANES[:LONG]])
    tops = [net.send(own.at[p + (top, first)], ext.at[p + (top, outer)], net.leftward) for p in PLANES]
    belows = [net.send(own.at[p + (top,)], ext.at[p + (outer, pl.ds(0, 2 * K))], net.over) for p in PLANES]
    lows = [net.send(own.at[p + (low, first)], ext.at[p + (low, outer)], net.leftward) for p in PLANES[LONG:]]
    for copy in inward:
        copy.wait()
    outward = [
        pltpu.make_async_copy(held.at[p], ext.at[p + (pl.ds(0, 2 * K), pl.ds(0, 2 * K))], ls.at[2 * p[0] + p[1]]) for p in PLANES
    ]
    for copy in outward:
        copy.start()
    corners = []

    def corner(n):
        tops[n].wait_recv()
        p = PLANES[n]
        corners.append(net.send(ext.at[p + (top, outer)], ext.at[p + (outer, outer)], net.over))

    def reorder(f):
        meas_out[f] = even_odd(meas[f], pick)

    fill_even_odd(pick)
    for copy in loads:
        copy.wait()
    for c in range(2):
        for half in range(2):
            beam_out[c, half] = probe[c, :, half * HALF : (half + 1) * HALF]
    relay.forward()
    corner(0)
    turned = even_odd(phase[...], pick)
    kern_out[0] = jnp.cos(turned)
    kern_out[1] = jnp.sin(turned)
    relay.forward()
    corner(1)
    reorder(0)
    relay.forward()
    corner(2)
    reorder(1)
    reorder(2)
    relay.forward()
    corner(3)
    reorder(3)
    for copy in belows + lows + corners + relay.hops:
        copy.wait_recv()
    for copy in outward:
        copy.wait()
    net.finish()


def run_open(own, phase, meas, probe):
    vmem = pl.BlockSpec(memory_space=pltpu.VMEM)
    anyw = pl.BlockSpec(memory_space=pl.ANY)
    shape = jax.ShapeDtypeStruct
    return pl.pallas_call(
        open_kernel,
        out_shape=[shape((2, 2, 3 * K, 3 * K), F32), shape((2, K, K), F32), shape(meas.shape, F32), shape((2, 2, K, HALF), F32)],
        in_specs=[anyw] * 4,
        out_specs=[anyw, vmem, vmem, vmem],
        scratch_shapes=[
            pltpu.VMEM((2, 2, 2 * K, 2 * K), F32),
            pltpu.VMEM((LONG, K, K), F32),
            pltpu.VMEM((LONG, K, K), F32),
            pltpu.VMEM(phase.shape, F32),
            pltpu.VMEM(meas.shape, F32),
            pltpu.VMEM((2, K, K), BF16),
            pltpu.VMEM(probe.shape, F32),
            pltpu.SemaphoreType.DMA((24,)),
            pltpu.SemaphoreType.DMA((24,)),
            pltpu.SemaphoreType.DMA((8,)),
        ],
        compiler_params=pltpu.CompilerParams(collective_id=2, has_side_effects=True, vmem_limit_bytes=51 << 20),
        cost_estimate=pl.CostEstimate(flops=20_000_000_000, bytes_accessed=24 << 20, transcendentals=0),
        name="open",
    )(own, phase, meas, probe)


def exchange_kernel(final, *refs):
    es, beam, g, ext, beam_new, new = refs[:6]
    gov, grv, ov, rx, rbl, from_left, tr = refs[6:13]
    rest = refs[13:]
    if final:
        way1, way2 = rest[:2]
        rest = rest[2:]
    else:
        rv, from_right, tl = rest[:3]
        rest = rest[3:]
    scale, rc, acc, rz, acc2, rxs, rys, total, ss, rs, ls = rest
    net = Net(ss, rs)
    core, x, y, z, partner, send = net.core, net.x, net.y, net.z, net.partner, net.send
    under, over, rightward, leftward = net.under, net.over, net.rightward, net.leftward

    def zpeer(d):
        zp = lax.rem(z + d, 4)
        return zp, ((zp * 4 + x) * 2 + core, y)

    def xpeer(d):
        xp = lax.rem(x + d, 4)
        return xp, ((z * 4 + xp) * 2 + core, y)

    def ypeer(d):
        yp = lax.rem(y + d, 4)
        return yp, (net.t, yp)

    whole, outer = pl.ds(0, 2 * K), pl.ds(2 * K, K)
    square, strip = (slice(None), slice(None), whole, whole), (slice(None), slice(None), whole, outer)
    local = [
        pltpu.make_async_copy(g.at[square], gov, ls.at[0]),
        pltpu.make_async_copy(g.at[strip], grv, ls.at[1]),
        pltpu.make_async_copy(ext.at[square], ov, ls.at[2]),
    ]
    if not final:
        local.append(pltpu.make_async_copy(ext.at[strip], rv, ls.at[3]))
    for copy in local:
        copy.start()
    net.meet([partner, under, over] + [p(d)[1] for p in (zpeer, xpeer, ypeer) for d in (1, 2, 3)])

    def reduce_steps():
        half, quarter, part = UNITS // 2, UNITS // 8, UNITS // 32
        copy = send(es.at[pl.ds((1 - core) * half, half)], rc, partner)
        yield
        copy.wait_recv()
        acc[...] = es[pl.ds(core * half, half)] + rc[...]
        copies = []
        for d in (1, 2, 3):
            zp, peer = zpeer(d)
            copies.append(send(acc.at[pl.ds(zp * quarter, quarter)], rz.at[d - 1], peer))
        yield
        for copy in copies:
            copy.wait_recv()
        acc2[...] = acc[pl.ds(z * quarter, quarter)] + (rz[0] + rz[1] + rz[2])
        copies = []
        for d in (1, 2, 3):
            xp, peer = xpeer(d)
            copies.append(send(acc2.at[pl.ds(xp * part, part)], rxs.at[d - 1], peer))
        yield
        for copy in copies:
            copy.wait_recv()
        rys[y] = acc2[pl.ds(x * part, part)] + (rxs[0] + rxs[1] + rxs[2])
        copies = [send(rys.at[y], rys.at[y], ypeer(d)[1]) for d in (1, 2, 3)]
        yield
        for copy in copies:
            copy.wait_recv()
        base = core * half + z * quarter + x * part
        total[pl.ds(base, part)] = (rys[0] + rys[1]) + (rys[2] + rys[3])
        for start, size, targets in (
            (base, part, [xpeer(d)[1] for d in (1, 2, 3)]),
            (core * half + z * quarter, quarter, [zpeer(d)[1] for d in (1, 2, 3)]),
            (core * half, half, [partner]),
        ):
            piece = total.at[pl.ds(start, size)]
            copies = [send(piece, piece, peer) for peer in targets]
            yield
            for copy in copies:
                copy.wait_recv()
        units = UNITS // 3
        for c in range(2):
            at = pl.ds(c * units, units)
            beam_new[at] = beam[at] - total[at] / (total[pl.ds(2 * units, units)] + 1.0)

    top, low = pl.ds(0, K), pl.ds(K, K)
    first, mid = pl.ds(0, K), pl.ds(K, K)

    def sweep(body):
        def step(i, carry):
            body(i * 32)
            return carry

        lax.fori_loop(0, K // 32, step, 0)

    def rows_at(base, i):
        return pl.ds(pl.multiple_of(base + i, 32), 32)

    corners, mids, lows, tops, ups, outs = {}, {}, {}, {}, [], []

    def down(p):
        corners[p] = (
            send(g.at[p + (outer, outer)], rx.at[p], under),
            send(g.at[p + (outer, first)], rbl.at[p + (slice(None), first)], under),
        )

    relays = []

    def start_relay(_):
        pieces = [(g.at[p + (low, outer)], from_left.at[p + (low,)]) for p in PLANES[:LONG]]
        relays.append(Relay(net, way1, way2, leftward, pieces))

    def forward(_):
        relays[0].forward()

    def bottom(p):
        lows[p] = [send(g.at[p + (low, outer)], from_left.at[p + (low,)], rightward)]
        if not final:
            lows[p].append(send(g.at[p + (low, first)], from_right.at[p + (low,)], leftward))

    def middle(p):
        mids[p] = send(g.at[p + (outer, mid)], rbl.at[p + (slice(None), mid)], under)

    def ready(_):
        for copy in local:
            copy.wait()
        units = UNITS // 3
        power = jnp.max(beam[pl.ds(0, units)] ** 2 + beam[pl.ds(units, units)] ** 2, axis=0)
        peak = jnp.max(jnp.max(power, axis=0, keepdims=True), axis=1, keepdims=True)
        scale[...] = jnp.broadcast_to(1.0 / peak, (8, K))

    def send_top(p):
        for copy in corners[p]:
            copy.wait_recv()

        def body(i):
            at = p + (rows_at(0, i),)
            tr[at] = grv[at] + rx[at]
            if not final:
                tl[at] = gov[at + (first,)] + rbl[at + (first,)]

        sweep(body)
        tops[p] = [send(tr.at[p], from_left.at[p + (top,)], rightward)]
        if not final:
            tops[p].append(send(tl.at[p], from_right.at[p + (top,)], leftward))

    def use_middle(p):
        mids[p].wait_recv()

        def body(i):
            inv = scale[0:1, :]
            at = p + (rows_at(0, i), mid)
            ov[at] = ov[at] - (gov[at] + rbl[at]) * inv
            at = p + (rows_at(K, i), mid)
            ov[at] = ov[at] - gov[at] * inv

        sweep(body)
        if not final:
            ups.append(send(ov.at[p + (top, mid)], new.at[p + (outer, mid)], over))

    def use_bottom(p):
        for copy in lows[p] if p in lows else [relays[0].hops[PLANES.index(p)]]:
            copy.wait_recv()

        def body(i):
            inv, at = scale[0:1, :], p + (rows_at(K, i),)
            ov[at + (first,)] = ov[at + (first,)] - (gov[at + (first,)] + from_left[at]) * inv
            if not final:
                rv[at] = rv[at] - (grv[at] + from_right[at]) * inv

        sweep(body)

    def use_top(p):
        for copy in tops[p]:
            copy.wait_recv()

        def body(i):
            inv, at = scale[0:1, :], p + (rows_at(0, i),)
            if final:
                mine = gov[at + (first,)] + rbl[at + (first,)]
            else:
                mine = tl[at]
                rv[at] = rv[at] - (tr[at] + from_right[at]) * inv
            ov[at + (first,)] = ov[at + (first,)] - (mine + from_left[at]) * inv

        sweep(body)
        n = len(outs)
        outs.append(pltpu.make_async_copy(ov.at[p], new.at[p + (whole, whole)], ls.at[4 + n]))
        if not final:
            ups.append(send(ov.at[p + (top, first)], new.at[p + (outer, first)], over))
            ups.append(send(rv.at[p + (top,)], new.at[p + (outer, outer)], over))
            outs.append(pltpu.make_async_copy(rv.at[p], new.at[p + (whole, outer)], ls.at[5 + n]))
        for copy in outs[n:]:
            copy.start()

    def settle(_):
        for copy in ups:
            copy.wait_recv()
        for copy in outs:
            copy.wait()

    reduce_run = reduce_steps()
    acts = {"d": down, "b": bottom, "m": middle, "L": ready, "t": send_top, "M": use_middle, "B": use_bottom, "T": use_top, "U": settle}
    if final:
        acts.update({"s": start_relay, "f": forward})
    done = {"b": LONG - 1, "B": LONG - 1, "T": LONG - 1} if final else {}
    for turn in ORDER[final]:
        if turn == "r":
            next(reduce_run, None)
        else:
            done[turn] = done.get(turn, -1) + 1
            acts[turn](PLANES[done[turn] % 4])
    for _ in reduce_run:
        pass
    net.finish()


def run_exchange(final, es, beam, grads, ext):
    tile = 2 * K
    vmem = pl.BlockSpec(memory_space=pltpu.VMEM)
    anyw = pl.BlockSpec(memory_space=pl.ANY)
    shape = jax.ShapeDtypeStruct
    square, strip = pltpu.VMEM((2, 2, tile, tile), F32), pltpu.VMEM((2, 2, tile, K), F32)
    flat, small = pltpu.VMEM((2, 2, K, tile), F32), pltpu.VMEM((2, 2, K, K), F32)
    scratch = [square, strip, square, small, flat, strip, small] + ([pltpu.VMEM((LONG, K, K), F32)] * 2 if final else [strip, strip, small])
    scratch += [
        pltpu.VMEM((8, K), F32),
        pltpu.VMEM((UNITS // 2, 8, HALF), F32),
        pltpu.VMEM((UNITS // 2, 8, HALF), F32),
        pltpu.VMEM((3, UNITS // 8, 8, HALF), F32),
        pltpu.VMEM((UNITS // 8, 8, HALF), F32),
        pltpu.VMEM((3, UNITS // 32, 8, HALF), F32),
        pltpu.VMEM((4, UNITS // 32, 8, HALF), F32),
        pltpu.VMEM((UNITS, 8, HALF), F32),
        pltpu.SemaphoreType.DMA((64,)),
        pltpu.SemaphoreType.DMA((64,)),
        pltpu.SemaphoreType.DMA((12,)),
    ]
    edge = tile if final else 3 * K
    return pl.pallas_call(
        functools.partial(exchange_kernel, final),
        out_shape=[shape(beam.shape, F32), shape((2, 2, edge, edge), F32)],
        in_specs=[vmem, vmem, anyw, anyw],
        out_specs=[vmem, anyw],
        scratch_shapes=scratch,
        compiler_params=pltpu.CompilerParams(
            collective_id=1 if final else 0, has_side_effects=True, vmem_limit_bytes=48 << 20
        ),
        cost_estimate=pl.CostEstimate(flops=20_000_000_000, bytes_accessed=24 << 20, transcendentals=0),
        name="close" if final else "exchange",
    )(es, beam, grads, ext)


def shards(object_field, probe, kernel_phase, measured, positions, batch):
    tables = constants()
    ext, kern, meas, beam = run_open(object_field, kernel_phase, measured, probe)
    for batch_no in range(BATCHES):
        grads, es = run_batch(batch_no, positions.T, batch, ext, beam, kern, meas, tables)
        flat, ext = run_exchange(
            batch_no + 1 == BATCHES, es.reshape(UNITS, 8, HALF), beam.reshape(UNITS * 2 // 3, 8, HALF), grads, ext
        )
        beam = flat.reshape(2, 2, K, HALF)
    return (ext, beam.transpose(0, 2, 1, 3).reshape(2, K, K))


def solution(mesh):
    in_specs = (
        P(None, None, "tile", "slab"),
        P(),
        P(),
        P(("tile", "slab"), None, None),
        P(("tile", "slab"), None),
        P(("tile", "slab")),
    )
    out_specs = (P(None, None, "tile", "slab"), P())
    return jax.shard_map(shards, mesh=mesh, in_specs=in_specs, out_specs=out_specs, check_vma=False)
```
